512 devices in a mesh: groups: 2 (over y), docs: 16 (over z), mp: 8 (over x), sub: 2 (over core).
Axes of the slice: x: 8, y: 2, z: 16, core: 2. Of those that a mesh axis runs over, the one named last changes fastest.
The devices are a block of a 8x8x16 slice.
Arguments:
- embeddings: bfloat16 [65536, 1024], P(('groups', 'docs', 'mp', 'sub')), parts along dimension 0, may hold values from -6 to 6
- owner_shard: int32 [65536, 1], P(('groups', 'docs', 'mp', 'sub')), parts along dimension 0, may hold values from 0 to 15; in each aligned block of 128 rows (0 to 127, 128 to 255, ...) at most 16 rows name the same one
- query_local: int32 [65536], P(('groups', 'docs', 'mp', 'sub')), parts along dimension 0, may hold values from 0 to 1
- labels: int32 [65536], P(('groups', 'docs', 'mp', 'sub')), parts along dimension 0, may hold values from 0 to 4
- w_first: bfloat16 [1024, 1024], replicated, may hold values from -0.1875 to 0.1875
- w_second: float32 [1024], replicated, may hold values from -0.1875 to 0.1875
Outputs:
- emb_grad: bfloat16 [65536, 1024], P(('groups', 'docs', 'mp', 'sub')), parts along dimension 0
- w_first_grad: float32 [2048, 1024], P(('groups', 'mp', 'sub')), parts along dimension 0
- w_second_grad: float32 [2048], P('groups'), parts along dimension 0
The draws below stay inside these ranges and needn't reach their ends.
There are 2 independent parts, one for each index of `groups`. The reference program is written for one: setup_inputs(seed, part) draws one part's arguments, and reference() takes and returns one part's arrays. A program takes and returns all parts, laid end to end along the dimension named above; an argument that names none is the same for every part. Nothing has to cross between parts.
Inputs may be any that keep to these rules, and one draw needn't show every extreme that they name: `owner_shard`: among the 128 rows of one document shard no owner appears more than 16 times, and some owner appears exactly 16 times.
All inputs are finite; a program needn't handle non-finite values.
Results may differ from the reference program's by a relative error of at most 0.017.
Values may be sent and summed in bfloat16 or wider, within the bound.
A program may use at most 64 MiB of HBM per device.

```python
import math
import jax
import jax.numpy as jnp
import numpy as np
from jax import lax

E = 1024
H = 1024
C_DEV = 128
Q_DEV = 2
CAND = 32768
CAP = 16
N_DOCS = 16
N_MP = 8
N_SUB = 2


def with_ends(entries, own_key, low, top_value):
    place = [jax.random.randint(jax.random.fold_in(own_key, axis), (), 0, length) for axis, length in enumerate(entries.shape)]
    main_axis = entries.shape.index(max(entries.shape))
    beside = place[:main_axis] + [(place[main_axis] + 1) % entries.shape[main_axis]] + place[main_axis + 1:]
    return entries.at[tuple(place)].set(low).at[tuple(beside)].set(top_value)


def shard_levels(own_key, dims, split, least, top_value):
    def one(axis_at, shards_of):
        heights = jax.random.uniform(jax.random.fold_in(jax.random.fold_in(own_key, 6), axis_at), (shards_of,), jnp.float32, least / len(split), top_value / len(split))
        return jnp.repeat(jnp.exp(heights), dims[axis_at] // shards_of).reshape((-1,) + (1,) * (len(dims) - axis_at - 1))

    loudness = one(*split[0])
    for cut in split[1:]:
        loudness = loudness * one(*cut)
    return loudness


def shared_out(key, own, number, rows, count, top, reach, lean):
    sequence = jax.random.permutation(key, count)
    packed, ordinary = shares(count, rows * top, reach, lean, True), shares(count, rows * top, reach, lean, False)
    places = jnp.arange(count)

    def named(tallies, offset_by):
        used = int((tallies > 0).sum())
        fixed = max(1, used // 4)
        shifted = fixed + (places - fixed + offset_by * (used - fixed)) % max(1, count - fixed)
        return jnp.zeros((count,), jnp.int32).at[sequence[jnp.where(places < fixed, places, shifted)]].set(jnp.asarray(tallies, jnp.int32))

    tallies = jnp.where(number % 4 == 0, named(packed, number // 4), named(ordinary, number - number // 4 - 1))
    mixed = jax.random.permutation(jax.random.fold_in(own, 3), count)
    giver, sink = mixed[0:count // 2 * 2:2], mixed[1:count // 2 * 2:2]
    margin = jnp.minimum(tallies[giver] - 1, reach - tallies[sink]) // 2
    margin = jnp.where((giver == sequence[0]) | (sink == sequence[0]) | (tallies[sink] == 0), 0, jnp.maximum(margin, 0))
    shifted = jax.random.randint(jax.random.fold_in(own, 4), (count // 2,), 0, 1 << 20) % (margin + 1)
    tallies = tallies.at[giver].add(-shifted).at[sink].add(shifted)
    items = jnp.searchsorted(jnp.cumsum(tallies), jnp.arange(rows * top), side="right").astype(jnp.int32)
    listing = items.reshape(top, rows).T
    listing = listing[jax.random.permutation(jax.random.fold_in(own, 1), rows)]
    offset_by = jax.random.randint(jax.random.fold_in(own, 2), (rows, 1), 0, top)
    return jnp.take_along_axis(listing, (jnp.arange(top)[None, :] + offset_by) % top, axis=1)


def shares(count, total, most, slope, full):
    portions = [(1 << 20) // math.isqrt(grade ** slope) + 1 for grade in range(1, count + 1)]
    largest = most if full else min(most, max(-(-total // count), total * portions[0] // sum(portions)))
    least = 1 if total - largest >= count - 1 else 0
    holding, rest = [largest] + [least] * (count - 1), total - largest - least * (count - 1)
    while rest > 0:
        movable = [i for i in range(1, count) if holding[i] < largest] or [i for i in range(1, count) if holding[i] < most]
        mass, left = sum([portions[i] for i in movable]), rest
        for i in movable:
            extra = min(most - holding[i], max(1, left * portions[i] // mass), rest)
            holding[i] = holding[i] + extra
            rest = rest - extra
    return np.array(holding)


def scatter_about(stream_key, extent, spread, most, pieces=(), held_as=jnp.bfloat16):
    result = jax.random.normal(stream_key, extent, jnp.float32) * spread
    if len(pieces) > 0:
        result = shard_levels(stream_key, extent, pieces, -0.22, 0.18) * result
    return jnp.clip(result, min=-most, max=most).astype(held_as)


def setup_inputs(seed: int = 0, part: int = 0) -> dict:
    streams_of = jax.random.split(jax.random.key(seed), 7)
    part_keys = jax.random.split(jax.random.fold_in(streams_of[6], part), 7)
    embeddings = scatter_about(part_keys[0], (CAND, E), 1.0, 6.0, ((0, 256),))
    owner_shard_keys = jax.random.split(jax.random.fold_in(part_keys[1], 1), CAND // C_DEV)
    owner_shard_turns = jax.random.permutation(jax.random.fold_in(part_keys[1], 3), CAND // C_DEV)
    owner_shard = jax.vmap(lambda own, number: shared_out(jax.random.fold_in(part_keys[1], 2), own, number, C_DEV, N_DOCS, 1, CAP, 2))(owner_shard_keys, owner_shard_turns).reshape((CAND, 1))
    query_local = with_ends(jax.random.randint(part_keys[2], (CAND,), 0, Q_DEV), jax.random.fold_in(part_keys[2], 1), 0, Q_DEV - 1).astype(jnp.int32)
    labels = with_ends(jax.random.randint(part_keys[3], (CAND,), 0, 5), jax.random.fold_in(part_keys[3], 1), 0, 4).astype(jnp.int32)
    w_first = scatter_about(streams_of[4], (E, H), E ** -0.5, 0.1875)
    w_second = scatter_about(streams_of[5], (H,), H ** -0.5, 0.1875, (), jnp.float32)
    return {"embeddings": embeddings, "owner_shard": owner_shard, "query_local": query_local, "labels": labels, "w_first": w_first, "w_second": w_second}


ranking_softness = 1.0


def silu_slope(pre_act):
    sigmoid_v = jax.nn.sigmoid(pre_act)
    return sigmoid_v * (1.0 + pre_act * (1.0 - sigmoid_v))


def rank_rows(row_start, row_count, scorer_outputs, query_mark, grade_slot):
    row_query = lax.dynamic_slice_in_dim(query_mark, row_start, row_count)
    single_row_score = lax.dynamic_slice_in_dim(scorer_outputs, row_start, row_count)
    row_label = lax.dynamic_slice_in_dim(grade_slot, row_start, row_count)
    slot_index = jnp.arange(scorer_outputs.shape[0], dtype=jnp.int32)
    row_index = row_start + jnp.arange(row_count, dtype=jnp.int32)
    matching_query = (row_query[:, None] == query_mark[None, :]) & (row_query[:, None] > 0)
    smooth_rank = jnp.sum(jnp.where(matching_query, jax.nn.sigmoid((scorer_outputs[None, :] - single_row_score[:, None]) / ranking_softness), 0.0), axis=1) - 0.5
    higher = (grade_slot[None, :] > row_label[:, None]) | ((grade_slot[None, :] == row_label[:, None]) & (slot_index[None, :] < row_index[:, None]))
    ideal_rank = jnp.sum((matching_query & higher).astype(jnp.float32), axis=1)
    row_gain = jnp.exp2(row_label.astype(jnp.float32)) - 1.0
    return smooth_rank, row_gain / jnp.log2(2.0 + ideal_rank)


def lambda_rows(row_start, row_count, scorer_outputs, query_mark, grade_slot, discount, inv_ideal):
    gain_all = jnp.exp2(grade_slot.astype(jnp.float32)) - 1.0
    row_query = lax.dynamic_slice_in_dim(query_mark, row_start, row_count)
    single_row_score = lax.dynamic_slice_in_dim(scorer_outputs, row_start, row_count)
    row_label = lax.dynamic_slice_in_dim(grade_slot, row_start, row_count)
    row_gain = lax.dynamic_slice_in_dim(gain_all, row_start, row_count)
    row_disc = lax.dynamic_slice_in_dim(discount, row_start, row_count)
    row_inv = lax.dynamic_slice_in_dim(inv_ideal, row_start, row_count)
    matching_query = (row_query[:, None] == query_mark[None, :]) & (row_query[:, None] > 0)
    score_gap = single_row_score[:, None] - scorer_outputs[None, :]
    weights = jnp.abs(row_gain[:, None] - gain_all[None, :]) * jnp.abs(row_disc[:, None] - discount[None, :]) * row_inv[:, None]
    direction = jnp.where(row_label[:, None] > grade_slot[None, :], -jax.nn.sigmoid(-score_gap), 0.0) + jnp.where(grade_slot[None, :] > row_label[:, None], jax.nn.sigmoid(score_gap), 0.0)
    return jnp.sum(jnp.where(matching_query, weights * direction, 0.0), axis=1)


def owner_lambdas(scorer_outputs, query_mark, grade_slot):
    slot_total = scorer_outputs.shape[0]
    row_count = math.gcd(slot_total, 512)
    starts = jnp.arange(0, slot_total, row_count, dtype=jnp.int32)

    def rank_block(first_row):
        return rank_rows(first_row, row_count, scorer_outputs, query_mark, grade_slot)

    smooth_rank, ideal_term = lax.map(rank_block, starts)
    smooth_rank = smooth_rank.reshape(slot_total)
    ideal_term = ideal_term.reshape(slot_total)
    discount = 1.0 / jnp.log2(2.0 + smooth_rank)
    member = (query_mark[:, None] == jnp.arange(1, Q_DEV + 1, dtype=jnp.int32)[None, :]).astype(jnp.float32)
    per_query = jnp.dot(ideal_term, member, precision=lax.Precision.HIGHEST)
    idcg = jnp.dot(member, per_query, precision=lax.Precision.HIGHEST)
    inv_ideal = jnp.where(idcg > 0.0, 1.0 / jnp.where(idcg > 0.0, idcg, 1.0), 0.0)

    def lambda_block(first_row):
        return lambda_rows(first_row, row_count, scorer_outputs, query_mark, grade_slot, discount, inv_ideal)

    return lax.map(lambda_block, starts).reshape(slot_total)


def owner_step(triple):
    return owner_lambdas(triple[0], triple[1], triple[2])


def reference(embeddings, owner_shard, query_local, labels, w_first, w_second):
    lanes = N_MP * N_SUB
    shards = N_DOCS * lanes
    slot_total = N_DOCS * CAP
    whole = shards * slot_total
    target = owner_shard[:, 0].astype(jnp.int32)
    hits = (target.reshape(shards, C_DEV)[:, :, None] == jnp.arange(N_DOCS, dtype=jnp.int32)[None, None, :]).astype(jnp.int32)
    before = (jnp.cumsum(hits, axis=1).astype(jnp.int32) - hits) * hits
    earlier = jnp.sum(before, axis=2).astype(jnp.int32).reshape(CAND)
    block_of = jnp.arange(CAND, dtype=jnp.int32) // C_DEV
    lane_of = block_of % lanes
    source_of = block_of // lanes
    slot_of = (((lane_of * N_DOCS + target) * N_DOCS + source_of) * CAP + earlier).astype(jnp.int32)
    emb_blocks = embeddings.reshape(shards, C_DEV, E)

    def forward(block):
        pre_act = jnp.dot(block, w_first, preferred_element_type=jnp.float32)
        hidden = pre_act * jax.nn.sigmoid(pre_act)
        return jnp.dot(hidden, w_second, precision=lax.Precision.HIGHEST)

    scorer_outputs = lax.map(forward, emb_blocks).reshape(CAND)
    query_mark = jnp.zeros((whole,), jnp.int32).at[slot_of].set(query_local.astype(jnp.int32) + 1)
    grade_slot = jnp.zeros((whole,), jnp.int32).at[slot_of].set(labels.astype(jnp.int32))
    score_slot = jnp.zeros((whole,), jnp.float32).at[slot_of].set(scorer_outputs)
    lambda_slot = lax.map(owner_step, (score_slot.reshape(shards, slot_total), query_mark.reshape(shards, slot_total), grade_slot.reshape(shards, slot_total)))
    lambdas = lambda_slot.reshape(whole)[slot_of]
    lambda_blocks = lambdas.reshape(shards, C_DEV)

    def backward(carry, pair):
        block, lambda_per_block = pair
        pre_act = jnp.dot(block, w_first, preferred_element_type=jnp.float32)
        hidden = pre_act * jax.nn.sigmoid(pre_act)
        pre_grad = (lambda_per_block[:, None] * w_second[None, :] * silu_slope(pre_act)).astype(jnp.bfloat16)
        emb_part = lax.dot_general(pre_grad, w_first, (((1,), (1,)), ((), ())), preferred_element_type=jnp.float32).astype(jnp.bfloat16)
        first = carry[0] + lax.dot_general(block, pre_grad, (((0,), (0,)), ((), ())), preferred_element_type=jnp.float32)
        second = carry[1] + jnp.dot(lambda_per_block, hidden, precision=lax.Precision.HIGHEST)
        return (first, second), emb_part

    start_carry = (jnp.zeros((E, H), jnp.float32), jnp.zeros((H,), jnp.float32))
    totals, emb_parts = lax.scan(backward, start_carry, (emb_blocks, lambda_blocks))
    return emb_parts.reshape(CAND, E), totals[0], totals[1]
```

```python
import functools
import math

import jax
import jax.numpy as jnp
from jax import lax
from jax.experimental import pallas as pl
from jax.experimental.pallas import tpu as pltpu
from jax.sharding import PartitionSpec as P

MESH = pl.DeviceIdType.MESH
F32 = jnp.float32
BF16 = jnp.bfloat16

NQ = 4
LN2 = math.log(2.0)
FWD = 4


def remote(src, dst, send_sem, recv_sem, where):
    return pltpu.make_async_remote_copy(
        src_ref=src, dst_ref=dst, send_sem=send_sem, recv_sem=recv_sem, device_id=where, device_id_type=MESH
    )


def by_distance(count):
    return sorted(range(1, count), key=lambda k: -min(k, count - k))


def step_kernel(
    nd, nm, rows, width, cap,
    emb_h, own_h, qry_h, lab_h, w1_h, w2_h,
    eg_h, wg_h, w2g_h,
    emb_v, own_v, qry_v, lab_v, w1_v, w2_v,
    slope_v, hid_v, hit_v,
    meta_s, meta_r, score_s, score_r,
    sa, sm, sg, sd, disc_v,
    embp_v, emb_t, pg, pg_in, g_v,
    x_s, x_r, z_s, z_r, z_f, ag_r, out_v, eg_v,
    w2_own, w2_x, w2_sum, w2_in, w2_z, w2_out,
    load_sem, out_sem, meta_ss, meta_rs, score_ss, score_rs,
    pair_ss, pair_rs, x_ss, x_rs, z_ss, z_rs, ag_ss, ag_rs,
    w2x_ss, w2x_rs, w2z_ss, w2z_rs,
):
    d = lax.axis_index("docs")
    m = lax.axis_index("mp")
    s = lax.axis_index("sub")
    other = 1 - s
    slots = nd * cap
    half = width // 2
    piece = half // NQ

    barrier = pltpu.get_barrier_semaphore()
    for k in by_distance(nd):
        for core in (s, other):
            pl.semaphore_signal(barrier, inc=1, device_id={"docs": lax.rem(d + k, nd), "sub": core}, device_id_type=MESH)
    for k in by_distance(nm):
        pl.semaphore_signal(barrier, inc=1, device_id={"mp": lax.rem(m + k, nm)}, device_id_type=MESH)
    pl.semaphore_signal(barrier, inc=1, device_id={"sub": other}, device_id_type=MESH)

    loads = [
        pltpu.make_async_copy(a, b, load_sem.at[i])
        for i, (a, b) in enumerate(
            ((own_h, own_v), (qry_h, qry_v), (lab_h, lab_v), (w2_h, w2_v), (emb_h, emb_v))
        )
    ]
    cols = width // FWD
    w_loads = [
        pltpu.make_async_copy(
            w1_h.at[:, pl.ds(i * cols, cols)], w1_v.at[:, pl.ds(i * cols, cols)], load_sem.at[5 + i]
        )
        for i in range(FWD)
    ]
    for copy in loads + w_loads:
        copy.start()

    for copy in loads[:3]:
        copy.wait()
    row_i = lax.broadcasted_iota(jnp.int32, (rows, rows), 0)
    col_i = lax.broadcasted_iota(jnp.int32, (rows, rows), 1)
    eye = row_i == col_i

    def upright(row):
        return jnp.sum(jnp.where(eye, row, 0.0), axis=1, keepdims=True)

    own_row = own_v[...].astype(F32)
    own_col = upright(own_row)
    earlier = jnp.sum(
        jnp.where((own_col == own_row) & (col_i < row_i), 1.0, 0.0), axis=1, keepdims=True
    )
    slot_col = own_col * cap + earlier
    hit = slot_col == lax.broadcasted_iota(jnp.int32, (rows, slots), 1).astype(F32)
    hit_v[...] = jnp.where(hit, 1.0, 0.0)

    def slotted(col):
        return jnp.sum(jnp.where(hit_v[...] > 0.0, col, 0.0), axis=0, keepdims=True)

    mark_own = slotted(upright(qry_v[...].astype(F32)) + 1.0)
    label_own = slotted(upright(lab_v[...].astype(F32)))
    meta_s[0:1, :] = mark_own.astype(BF16)
    meta_s[1:2, :] = label_own.astype(BF16)
    meta_r[d, 0:1, :] = mark_own.astype(BF16)
    meta_r[d, 1:2, :] = label_own.astype(BF16)

    for copy in loads[3:]:
        copy.wait()
    score = jnp.zeros((rows, 1), F32)
    for i in range(FWD):
        w_loads[i].wait()
        at = pl.ds(i * cols, cols)
        pre = jnp.dot(emb_v[...], w1_v[:, at], preferred_element_type=F32)
        sig = 0.5 + 0.5 * jnp.tanh(0.5 * pre)
        hid = pre * sig
        w2 = w2_v[:, at]
        hid_v[:, at] = hid
        score += jnp.sum(hid * w2, axis=1, keepdims=True)
        slope_v[:, at] = w2 * (sig * (1.0 + pre * (1.0 - sig)))
    score_own = slotted(0.5 * score)
    score_s[...] = score_own
    score_r[d] = score_own

    pl.semaphore_wait(barrier, 2 * (nd - 1) + (nm - 1) + 1)

    score_sends, meta_sends = [], []
    for k in by_distance(nd):
        where = {"docs": lax.rem(d + k, nd)}
        meta_sends.append(remote(meta_s, meta_r.at[d], meta_ss.at[k], meta_rs.at[d], where))
        meta_sends[-1].start()
        score_sends.append(remote(score_s, score_r.at[d], score_ss.at[k], score_rs.at[d], where))
        score_sends[-1].start()
    emb_send = remote(emb_v, embp_v, pair_ss.at[0], pair_rs.at[0], {"sub": other})
    emb_send.start()

    def turn(block, at):
        for c in range(nm):
            w = width // nm
            emb_t[c, :, at * rows : (at + 1) * rows] = (
                block[:, c * w : (c + 1) * w].astype(F32).T.astype(BF16)
            )

    turn(emb_v, 0)
    emb_send.wait_recv()
    turn(embp_v, 1)

    for k in by_distance(nd):
        src = lax.rem(d + k, nd)
        remote(meta_s, meta_r.at[src], meta_ss.at[k], meta_rs.at[src], {"docs": src}).wait_recv()
    lane = lax.broadcasted_iota(jnp.int32, (nd, slots), 1)
    in_group = lax.rem(lane, cap)

    def turned(a, by):
        near = pltpu.roll(a, by, 1)
        far = pltpu.roll(a, by + slots - cap, 1)
        return jnp.where(in_group >= by, near, far)

    mark = jnp.concatenate([meta_r[i, 0:1, :].astype(F32) for i in range(nd)], axis=0)
    label = jnp.concatenate([meta_r[i, 1:2, :].astype(F32) for i in range(nd)], axis=0)
    gain = jnp.exp2(label) - 1.0
    sm[0] = mark
    sg[0] = gain

    for by in range(1, cap):
        sm[by] = turned(mark, by)
        sg[by] = turned(gain, by)

    group_r = lax.broadcasted_iota(jnp.int32, (slots, slots), 0) // cap
    group_c = lax.broadcasted_iota(jnp.int32, (slots, slots), 1) // cap
    groups = jnp.where(group_r == group_c, 1.0, 0.0).astype(BF16)
    tallies = []
    for q in (1.0, 2.0):
        for least in range(5):
            tallies.append(
                jnp.sum(jnp.where((mark == q) & (label >= float(least)), 1.0, 0.0), axis=0, keepdims=True)
            )
    tallies += [jnp.zeros((6, slots), F32)]
    counts = jnp.dot(jnp.concatenate(tallies, axis=0).astype(BF16), groups, preferred_element_type=F32)
    total = jnp.where(mark == 1.0, counts[0:1], counts[5:6])
    at_least = jnp.where(mark_own == 1.0, counts[1:5], counts[6:10])

    def rank_weight(r, acc):
        r = r.astype(F32)
        w = LN2 / jnp.log(jnp.full((4, slots), 2.0, F32) + r)
        return acc + jnp.where(at_least > r, w, 0.0)

    ladder = lax.fori_loop(0, slots, rank_weight, jnp.zeros((4, slots), F32), unroll=8)
    idcg = ladder[0:1] + 2.0 * ladder[1:2] + 4.0 * ladder[2:3] + 8.0 * ladder[3:4]
    inv = jnp.where(idcg > 0.0, 1.0 / jnp.where(idcg > 0.0, idcg, 1.0), 0.0)
    gain_own = jnp.exp2(label_own) - 1.0

    for k in by_distance(nd):
        src = lax.rem(d + k, nd)
        remote(score_s, score_r.at[src], score_ss.at[k], score_rs.at[src], {"docs": src}).wait_recv()
    scores = jnp.concatenate([score_r[i] for i in range(nd)], axis=0)
    sa[0] = scores
    for by in range(1, cap):
        sa[by] = turned(scores, by)

    def soft(by, acc):
        for j in range(nd):
            t = jnp.tanh(sa[by, j : j + 1, :] - scores)
            acc += jnp.where(sm[by, j : j + 1, :] == mark, t, 0.0)
        return acc

    acc = lax.fori_loop(0, cap, soft, jnp.zeros((nd, slots), F32))
    rank = jnp.where(mark > 0.0, 0.5 * (total - 1.0 + acc), 0.0)
    disc = LN2 / jnp.log(2.0 + rank)
    disc_v[...] = disc
    disc_own = disc_v[pl.ds(d, 1), :]
    sd[0] = disc
    for by in range(1, cap):
        sd[by] = turned(disc, by)

    def pairs(by, acc):
        t = jnp.tanh(sa[by] - score_own)
        gap = sg[by] - gain_own
        term = jnp.abs(sd[by] - disc_own) * (gap - jnp.abs(gap) * t)
        return acc + jnp.where(sm[by] == mark_own, term, 0.0)

    acc = lax.fori_loop(0, cap, pairs, jnp.zeros((nd, slots), F32), unroll=2)
    lam_row = 0.5 * inv * jnp.sum(acc, axis=0, keepdims=True)
    lam = jnp.sum(jnp.where(hit_v[...] > 0.0, lam_row, 0.0), axis=1, keepdims=True)

    for h in range(2):
        pg[h] = (lam * slope_v[:, h * half : (h + 1) * half]).astype(BF16)
    pg_send = remote(pg.at[other], pg_in, pair_ss.at[1], pair_rs.at[1], {"sub": other})
    pg_send.start()
    for i in range(width // 128):
        w2_own[i : i + 1, :] = jnp.sum(lam * hid_v[:, i * 128 : (i + 1) * 128], axis=0, keepdims=True)
    w2_x[m] = w2_own[...]
    pg_send.wait_recv()
    both = jnp.concatenate([pg[s], pg_in[...]], axis=0)

    right, left = {"mp": lax.rem(m + 1, nm)}, {"mp": lax.rem(m + nm - 1, nm)}
    far = nm // 2

    def product(rel):
        g_v[rel] = jnp.dot(emb_t[lax.rem(m + rel, nm)], both, preferred_element_type=F32)

    x_sends = []

    def ring_send(side, step, q, value):
        x_s[side, step, q] = value.astype(BF16)
        copy = remote(
            x_s.at[side, step, q], x_r.at[side, step, q], x_ss.at[side, step, q], x_rs.at[side, step, q],
            (right, left)[side],
        )
        copy.start()
        x_sends.append(copy)

    def ring_recv(side, step, q):
        remote(
            x_s.at[side, step, q], x_r.at[side, step, q], x_ss.at[side, step, q], x_rs.at[side, step, q],
            (right, left)[side],
        ).wait_recv()
        return x_r[side, step, q].astype(F32)

    def own(rel, q):
        return g_v[rel, :, q * piece : (q + 1) * piece]

    def rel_of(side, step):
        away = far - step
        return away if side == 0 else (nm - away) % nm

    def long_way(side, q):
        return (q < NQ // 2) == (side == 0)

    product(far)
    for side in range(2):
        for q in range(NQ):
            if long_way(side, q):
                ring_send(side, 0, q, own(far, q))
    for side in range(2):
        product(rel_of(side, 1))
        for q in range(NQ):
            if not long_way(side, q):
                ring_send(side, 1, q, own(rel_of(side, 1), q))
    for step in range(2, far):
        for side in range(2):
            product(rel_of(side, step))
    product(0)

    w2x_sends = []
    for k in by_distance(nm):
        copy = remote(w2_own, w2_x.at[m], w2x_ss.at[k], w2x_rs.at[m], {"mp": lax.rem(m + k, nm)})
        copy.start()
        w2x_sends.append(copy)

    order = list(range(NQ))
    for q in order:
        for side in range(2):
            if long_way(side, q):
                ring_send(side, 1, q, ring_recv(side, 0, q) + own(rel_of(side, 1), q))
    for step in range(2, far):
        for q in order:
            for side in range(2):
                ring_send(side, step, q, ring_recv(side, step - 1, q) + own(rel_of(side, step), q))

    for k in by_distance(nm):
        src = lax.rem(m + k, nm)
        remote(w2_own, w2_x.at[src], w2x_ss.at[k], w2x_rs.at[src], {"mp": src}).wait_recv()
    w2_sum[0] = functools.reduce(lambda a, b: a + b, [w2_x[i] for i in range(nm)])
    w2_pair = remote(w2_sum.at[0], w2_in, pair_ss.at[2], pair_rs.at[2], {"sub": other})
    w2_pair.start()

    z_sends = []
    for q in order:
        block = own(0, q)
        for side in range(2):
            block = block + ring_recv(side, far - 1, q)
        z_s[q] = block.reshape(nd // 2, 16, piece).astype(BF16)
        z, par = q // 2, q % 2

        @pl.when(lax.rem(d, 2) == par)
        def _():
            z_r[z, d] = z_s[q, d // 2]

        for k in by_distance(nd):
            to = lax.rem(d + k, nd)
            copy = remote(z_s.at[q, to // 2], z_r.at[z, d], z_ss.at[z, k], z_rs.at[z, d], {"docs": to})
            z_sends.append((copy, to, par))
            pl.when(lax.rem(to, 2) == par)(copy.start)
        if q == 1:
            w2_pair.wait_recv()
            w2_sum[1] = w2_sum[0] + w2_in[...]
            w2_z[d] = w2_sum[1]
            w2z_sends = []
            for k in by_distance(nd):
                copy = remote(
                    w2_sum.at[1], w2_z.at[d], w2z_ss.at[k], w2z_rs.at[d], {"docs": lax.rem(d + k, nd)}
                )
                copy.start()
                w2z_sends.append(copy)

    grad = lax.dot_general(
        pg[0], w1_v[:, :half], (((1,), (1,)), ((), ())), preferred_element_type=F32
    ) + lax.dot_general(pg[1], w1_v[:, half:], (((1,), (1,)), ((), ())), preferred_element_type=F32)
    eg_v[...] = grad.astype(BF16)
    eg_out = pltpu.make_async_copy(eg_v, eg_h, out_sem.at[0])
    eg_out.start()
    return (
        d, m, s, other, nd, cap, half, z_sends, w2z_sends, x_sends, w2x_sends, score_sends, meta_sends,
        emb_send, pg_send, w2_pair, eg_out,
    )


def whole_kernel(nd, nm, rows, width, cap, *refs):
    state = step_kernel(nd, nm, rows, width, cap, *refs)
    (
        d, m, s, other, nd, cap, half, z_sends, w2z_sends, x_sends, w2x_sends, score_sends, meta_sends,
        emb_send, pg_send, w2_pair, eg_out,
    ) = state
    (
        emb_h, own_h, qry_h, lab_h, w1_h, w2_h,
        eg_h, wg_h, w2g_h,
        emb_v, own_v, qry_v, lab_v, w1_v, w2_v,
        slope_v, hid_v, hit_v,
        meta_s, meta_r, score_s, score_r,
        sa, sm, sg, sd, disc_v,
        embp_v, emb_t, pg, pg_in, g_v,
        x_s, x_r, z_s, z_r, z_f, ag_r, out_v, eg_v,
        w2_own, w2_x, w2_sum, w2_in, w2_z, w2_out,
        load_sem, out_sem, meta_ss, meta_rs, score_ss, score_rs,
        pair_ss, pair_rs, x_ss, x_rs, z_ss, z_rs, ag_ss, ag_rs,
        w2x_ss, w2x_rs, w2z_ss, w2z_rs,
    ) = refs
    part = nd // 2
    core = d // part
    mine = lax.rem(d, part)
    ag_sends = []
    for z in range(2):
        for k in by_distance(nd):
            src = lax.rem(d + k, nd)
            remote(z_s.at[0, 0], z_r.at[z, src], z_ss.at[z, k], z_rs.at[z, src], {"docs": src}).wait_recv()
        z_f[z] = functools.reduce(lambda a, b: a + b, [z_r[z, i].astype(F32) for i in range(nd)]).astype(BF16)

        @pl.when(core == s)
        def _():
            ag_r[s, z, mine] = z_f[z]

        for k in by_distance(nd) + [0]:
            copy = remote(
                z_f.at[z], ag_r.at[s, z, mine], ag_ss.at[z, k], ag_rs.at[s, z, mine],
                {"docs": lax.rem(d + k, nd), "sub": core},
            )
            if k == 0:
                pl.when(core != s)(copy.start)
            else:
                copy.start()
            ag_sends.append((copy, k))

    for k in by_distance(nd):
        src = lax.rem(d + k, nd)
        remote(w2_sum.at[1], w2_z.at[src], w2z_ss.at[k], w2z_rs.at[src], {"docs": src}).wait_recv()
    w2_out[...] = functools.reduce(lambda a, b: a + b, [w2_z[i] for i in range(nd)])
    w2_copy = pltpu.make_async_copy(w2_out, w2g_h, out_sem.at[1])
    w2_copy.start()

    for z in range(2):
        for src in range(2):
            for k in range(part):
                copy = remote(
                    z_f.at[z], ag_r.at[src, z, k], ag_ss.at[z, k], ag_rs.at[src, z, k], {"sub": other}
                )
                same = (src == s) & (s * part + k == d)
                pl.when(jnp.logical_not(same))(copy.wait_recv)
                out_v[(k // 2) * 16 : (k // 2) * 16 + 16, pl.ds(src * half + z * 256 + (k % 2) * 128, 128)] = ag_r[
                    src, z, k
                ].astype(F32)
    wg_copy = pltpu.make_async_copy(out_v, wg_h, out_sem.at[2])
    wg_copy.start()

    for copy in score_sends + meta_sends + [emb_send, pg_send, w2_pair] + x_sends + w2x_sends + w2z_sends:
        copy.wait_send()
    for copy, to, par in z_sends:
        pl.when(lax.rem(to, 2) == par)(copy.wait_send)
    for copy, k in ag_sends:
        if k == 0:
            pl.when(core != s)(copy.wait_send)
        else:
            copy.wait_send()
    eg_out.wait()
    w2_copy.wait()
    wg_copy.wait()


def solution(mesh):
    nd, nm = mesh.shape["docs"], mesh.shape["mp"]

    def on_device(embeddings, owner_shard, query_local, labels, w_first, w_second):
        rows, width = embeddings.shape
        cap = 2 * rows // nd
        slots = nd * cap
        half = width // 2
        piece = half // NQ
        far = nm // 2
        dma = pltpu.SemaphoreType.DMA
        any_spec = pl.BlockSpec(memory_space=pl.ANY)
        scratch = [
            pltpu.VMEM((rows, width), BF16),
            pltpu.VMEM((1, rows), jnp.int32),
            pltpu.VMEM((1, rows), jnp.int32),
            pltpu.VMEM((1, rows), jnp.int32),
            pltpu.VMEM((width, width), BF16),
            pltpu.VMEM((1, width), F32),
            pltpu.VMEM((rows, width), F32),
            pltpu.VMEM((rows, width), F32),
            pltpu.VMEM((rows, slots), F32),
            pltpu.VMEM((2, slots), BF16),
            pltpu.VMEM((nd, 2, slots), BF16),
            pltpu.VMEM((1, slots), F32),
            pltpu.VMEM((nd, 1, slots), F32),
            pltpu.VMEM((cap, nd, slots), F32),
            pltpu.VMEM((cap, nd, slots), F32),
            pltpu.VMEM((cap, nd, slots), F32),
            pltpu.VMEM((cap, nd, slots), F32),
            pltpu.VMEM((nd, slots), F32),
            pltpu.VMEM((rows, width), BF16),
            pltpu.VMEM((nm, width // nm, 2 * rows), BF16),
            pltpu.VMEM((2, rows, half), BF16),
            pltpu.VMEM((rows, half), BF16),
            pltpu.VMEM((nm, width // nm, half), F32),
            pltpu.VMEM((2, far, NQ, width // nm, piece), BF16),
            pltpu.VMEM((2, far, NQ, width // nm, piece), BF16),
            pltpu.VMEM((NQ, nd // 2, 16, piece), BF16),
            pltpu.VMEM((2, nd, 16, piece), BF16),
            pltpu.VMEM((2, 16, piece), BF16),
            pltpu.VMEM((2, 2, nd // 2, 16, piece), BF16),
            pltpu.VMEM((width // nm // 2, width), F32),
            pltpu.VMEM((rows, width), BF16),
            pltpu.VMEM((width // 128, 128), F32),
            pltpu.VMEM((nm, width // 128, 128), F32),
            pltpu.VMEM((2, width // 128, 128), F32),
            pltpu.VMEM((width // 128, 128), F32),
            pltpu.VMEM((nd, width // 128, 128), F32),
            pltpu.VMEM((width // 128, 128), F32),
            dma((5 + FWD,)),
            dma((3,)),
            dma((nd,)),
            dma((nd,)),
            dma((nd,)),
            dma((nd,)),
            dma((3,)),
            dma((3,)),
            dma((2, far, NQ)),
            dma((2, far, NQ)),
            dma((2, nd)),
            dma((2, nd)),
            dma((2, nd)),
            dma((2, 2, nd // 2)),
            dma((nm,)),
            dma((nm,)),
            dma((nd,)),
            dma((nd,)),
        ]
        emb_grad, w_first_grad, w_second_grad = pl.pallas_call(
            functools.partial(whole_kernel, nd, nm, rows, width, cap),
            out_shape=(
                jax.ShapeDtypeStruct((rows, width), BF16),
                jax.ShapeDtypeStruct((width // nm // 2, width), F32),
                jax.ShapeDtypeStruct((width // 128, 128), F32),
            ),
            in_specs=[any_spec] * 6,
            out_specs=(any_spec,) * 3,
            scratch_shapes=scratch,
            compiler_params=pltpu.CompilerParams(
                collective_id=0, has_side_effects=True, vmem_limit_bytes=48 * 1024 * 1024
            ),
            name="ranking_step",
        )(
            embeddings,
            owner_shard.reshape(1, rows),
            query_local.reshape(1, rows),
            labels.reshape(1, rows),
            w_first,
            w_second.reshape(1, width),
        )
        return emb_grad, w_first_grad, w_second_grad.reshape(width)

    whole = ("groups", "docs", "mp", "sub")
    return jax.shard_map(
        on_device,
        mesh=mesh,
        in_specs=(P(whole, None), P(whole, None), P(whole), P(whole), P(), P()),
        out_specs=(P(whole, None), P(("groups", "mp", "sub"), None), P("groups")),
        check_vma=False,
    )
```

```python
import functools
import math

import jax
import jax.numpy as jnp
from jax import lax
from jax.experimental import pallas as pl
from jax.experimental.pallas import tpu as pltpu
from jax.sharding import PartitionSpec as P

MESH = pl.DeviceIdType.MESH
F32 = jnp.float32
BF16 = jnp.bfloat16

NQ = 4
LN2 = math.log(2.0)
FWD = 4


def remote(src, dst, send_sem, recv_sem, where):
    return pltpu.make_async_remote_copy(
        src_ref=src, dst_ref=dst, send_sem=send_sem, recv_sem=recv_sem, device_id=where, device_id_type=MESH
    )


class Phases:
    def __init__(self):
        self.scope = None

    def __call__(self, name):
        if self.scope is not None:
            self.scope.__exit__(None, None, None)
        self.scope = jax.named_scope(name) if name else None
        if self.scope is not None:
            self.scope.__enter__()


def by_distance(count):
    return sorted(range(1, count), key=lambda k: -min(k, count - k))


def step_kernel(
    nd, nm, rows, width, cap,
    emb_h, own_h, qry_h, lab_h, w1_h, w2_h,
    eg_v, out_v, w2_out,
    emb_v, own_v, qry_v, lab_v, w1_v, w2_v,
    slope_v, hid_v, hit_v,
    meta_s, meta_r, score_s, score_r,
    sa, sm, sg, sd, disc_v,
    embp_v, emb_t, pg, pg_in, g_v,
    x_s, x_r, z_s, z_r, z_f, ag_r,
    w2_own, w2_x, w2_sum, w2_in, w2_z,
    load_sem, meta_ss, meta_rs, score_ss, score_rs,
    pair_ss, pair_rs, x_ss, x_rs, z_ss, z_rs, ag_ss, ag_rs,
    w2x_ss, w2x_rs, w2z_ss, w2z_rs,
):
    d = lax.axis_index("docs")
    m = lax.axis_index("mp")
    s = lax.axis_index("sub")
    other = 1 - s
    slots = nd * cap
    half = width // 2
    piece = half // NQ

    phase = Phases()
    phase("greet")
    barrier = pltpu.get_barrier_semaphore()
    for k in by_distance(nd):
        for core in (s, other):
            pl.semaphore_signal(barrier, inc=1, device_id={"docs": lax.rem(d + k, nd), "sub": core}, device_id_type=MESH)
    for k in by_distance(nm):
        pl.semaphore_signal(barrier, inc=1, device_id={"mp": lax.rem(m + k, nm)}, device_id_type=MESH)
    pl.semaphore_signal(barrier, inc=1, device_id={"sub": other}, device_id_type=MESH)

    loads = [
        pltpu.make_async_copy(a, b, load_sem.at[i])
        for i, (a, b) in enumerate(
            ((own_h, own_v), (qry_h, qry_v), (lab_h, lab_v), (w2_h, w2_v), (emb_h, emb_v))
        )
    ]
    cols = width // FWD
    w_loads = [
        pltpu.make_async_copy(
            w1_h.at[:, pl.ds(i * cols, cols)], w1_v.at[:, pl.ds(i * cols, cols)], load_sem.at[5 + i]
        )
        for i in range(FWD)
    ]
    for copy in loads + w_loads:
        copy.start()

    phase("own_slots")
    for copy in loads[:3]:
        copy.wait()
    row_i = lax.broadcasted_iota(jnp.int32, (rows, rows), 0)
    col_i = lax.broadcasted_iota(jnp.int32, (rows, rows), 1)
    eye = row_i == col_i

    def upright(row):
        return jnp.sum(jnp.where(eye, row, 0.0), axis=1, keepdims=True)

    own_row = own_v[...].astype(F32)
    own_col = upright(own_row)
    earlier = jnp.sum(
        jnp.where((own_col == own_row) & (col_i < row_i), 1.0, 0.0), axis=1, keepdims=True
    )
    slot_col = own_col * cap + earlier
    hit = slot_col == lax.broadcasted_iota(jnp.int32, (rows, slots), 1).astype(F32)
    hit_v[...] = jnp.where(hit, 1.0, 0.0)

    def slotted(col):
        return jnp.sum(jnp.where(hit_v[...] > 0.0, col, 0.0), axis=0, keepdims=True)

    mark_own = slotted(upright(qry_v[...].astype(F32)) + 1.0)
    label_own = slotted(upright(lab_v[...].astype(F32)))
    meta_s[0:1, :] = mark_own.astype(BF16)
    meta_s[1:2, :] = label_own.astype(BF16)
    meta_r[d, 0:1, :] = mark_own.astype(BF16)
    meta_r[d, 1:2, :] = label_own.astype(BF16)

    phase("scorer")
    for copy in loads[3:]:
        copy.wait()
    score = jnp.zeros((rows, 1), F32)
    for i in range(FWD):
        w_loads[i].wait()
        at = pl.ds(i * cols, cols)
        pre = jnp.dot(emb_v[...], w1_v[:, at], preferred_element_type=F32)
        sig = 0.5 + 0.5 * jnp.tanh(0.5 * pre)
        hid = pre * sig
        w2 = w2_v[:, at]
        hid_v[:, at] = hid
        score += jnp.sum(hid * w2, axis=1, keepdims=True)
        slope_v[:, at] = w2 * (sig * (1.0 + pre * (1.0 - sig)))
    score_own = slotted(0.5 * score)
    score_s[...] = score_own
    score_r[d] = score_own

    phase("barrier")
    pl.semaphore_wait(barrier, 2 * (nd - 1) + (nm - 1) + 1)

    phase("send_scores")
    score_sends, meta_sends = [], []
    for k in by_distance(nd):
        where = {"docs": lax.rem(d + k, nd)}
        meta_sends.append(remote(meta_s, meta_r.at[d], meta_ss.at[k], meta_rs.at[d], where))
        meta_sends[-1].start()
        score_sends.append(remote(score_s, score_r.at[d], score_ss.at[k], score_rs.at[d], where))
        score_sends[-1].start()
    emb_send = remote(emb_v, embp_v, pair_ss.at[0], pair_rs.at[0], {"sub": other})
    emb_send.start()

    phase("turn")
    def turn(block, at):
        for c in range(nm):
            w = width // nm
            emb_t[c, :, at * rows : (at + 1) * rows] = (
                block[:, c * w : (c + 1) * w].astype(F32).T.astype(BF16)
            )

    turn(emb_v, 0)
    emb_send.wait_recv()
    turn(embp_v, 1)

    phase("meta_wait")
    for k in by_distance(nd):
        src = lax.rem(d + k, nd)
        remote(meta_s, meta_r.at[src], meta_ss.at[k], meta_rs.at[src], {"docs": src}).wait_recv()
    phase("meta_work")
    lane = lax.broadcasted_iota(jnp.int32, (nd, slots), 1)
    in_group = lax.rem(lane, cap)

    def turned(a, by):
        near = pltpu.roll(a, by, 1)
        far = pltpu.roll(a, by + slots - cap, 1)
        return jnp.where(in_group >= by, near, far)

    mark = jnp.concatenate([meta_r[i, 0:1, :].astype(F32) for i in range(nd)], axis=0)
    label = jnp.concatenate([meta_r[i, 1:2, :].astype(F32) for i in range(nd)], axis=0)
    gain = jnp.exp2(label) - 1.0
    sm[0] = mark
    sg[0] = gain

    for by in range(1, cap):
        sm[by] = turned(mark, by)
        sg[by] = turned(gain, by)

    group_r = lax.broadcasted_iota(jnp.int32, (slots, slots), 0) // cap
    group_c = lax.broadcasted_iota(jnp.int32, (slots, slots), 1) // cap
    groups = jnp.where(group_r == group_c, 1.0, 0.0).astype(BF16)
    tallies = []
    for q in (1.0, 2.0):
        for least in range(5):
            tallies.append(
                jnp.sum(jnp.where((mark == q) & (label >= float(least)), 1.0, 0.0), axis=0, keepdims=True)
            )
    tallies += [jnp.zeros((6, slots), F32)]
    counts = jnp.dot(jnp.concatenate(tallies, axis=0).astype(BF16), groups, preferred_element_type=F32)
    total = jnp.where(mark == 1.0, counts[0:1], counts[5:6])
    at_least = jnp.where(mark_own == 1.0, counts[1:5], counts[6:10])

    def rank_weight(r, acc):
        r = r.astype(F32)
        w = LN2 / jnp.log(jnp.full((4, slots), 2.0, F32) + r)
        return acc + jnp.where(at_least > r, w, 0.0)

    ladder = lax.fori_loop(0, slots, rank_weight, jnp.zeros((4, slots), F32), unroll=8)
    idcg = ladder[0:1] + 2.0 * ladder[1:2] + 4.0 * ladder[2:3] + 8.0 * ladder[3:4]
    inv = jnp.where(idcg > 0.0, 1.0 / jnp.where(idcg > 0.0, idcg, 1.0), 0.0)
    gain_own = jnp.exp2(label_own) - 1.0

    phase("score_wait")
    for k in by_distance(nd):
        src = lax.rem(d + k, nd)
        remote(score_s, score_r.at[src], score_ss.at[k], score_rs.at[src], {"docs": src}).wait_recv()
    phase("soft_rank")
    scores = jnp.concatenate([score_r[i] for i in range(nd)], axis=0)
    sa[0] = scores
    for by in range(1, cap):
        sa[by] = turned(scores, by)

    def soft(by, acc):
        for j in range(nd):
            t = jnp.tanh(sa[by, j : j + 1, :] - scores)
            acc += jnp.where(sm[by, j : j + 1, :] == mark, t, 0.0)
        return acc

    acc = lax.fori_loop(0, cap, soft, jnp.zeros((nd, slots), F32))
    rank = jnp.where(mark > 0.0, 0.5 * (total - 1.0 + acc), 0.0)
    disc = LN2 / jnp.log(2.0 + rank)
    disc_v[...] = disc
    disc_own = disc_v[pl.ds(d, 1), :]
    sd[0] = disc
    for by in range(1, cap):
        sd[by] = turned(disc, by)

    phase("lambdas")
    def pairs(by, acc):
        t = jnp.tanh(sa[by] - score_own)
        gap = sg[by] - gain_own
        term = jnp.abs(sd[by] - disc_own) * (gap - jnp.abs(gap) * t)
        return acc + jnp.where(sm[by] == mark_own, term, 0.0)

    acc = lax.fori_loop(0, cap, pairs, jnp.zeros((nd, slots), F32), unroll=2)
    lam_row = 0.5 * inv * jnp.sum(acc, axis=0, keepdims=True)
    lam = jnp.sum(jnp.where(hit_v[...] > 0.0, lam_row, 0.0), axis=1, keepdims=True)

    phase("pre_grad")
    for h in range(2):
        pg[h] = (lam * slope_v[:, h * half : (h + 1) * half]).astype(BF16)
    pg_send = remote(pg.at[other], pg_in, pair_ss.at[1], pair_rs.at[1], {"sub": other})
    pg_send.start()
    for i in range(width // 128):
        w2_own[i : i + 1, :] = jnp.sum(lam * hid_v[:, i * 128 : (i + 1) * 128], axis=0, keepdims=True)
    w2_x[m] = w2_own[...]
    phase("pair_wait")
    pg_send.wait_recv()
    both = jnp.concatenate([pg[s], pg_in[...]], axis=0)

    right, left = {"mp": lax.rem(m + 1, nm)}, {"mp": lax.rem(m + nm - 1, nm)}
    far = nm // 2

    def product(rel):
        g_v[rel] = jnp.dot(emb_t[lax.rem(m + rel, nm)], both, preferred_element_type=F32)

    x_sends = []

    def ring_send(side, step, q, value):
        x_s[side, step, q] = value.astype(BF16)
        copy = remote(
            x_s.at[side, step, q], x_r.at[side, step, q], x_ss.at[side, step, q], x_rs.at[side, step, q],
            (right, left)[side],
        )
        copy.start()
        x_sends.append(copy)

    def ring_recv(side, step, q):
        remote(
            x_s.at[side, step, q], x_r.at[side, step, q], x_ss.at[side, step, q], x_rs.at[side, step, q],
            (right, left)[side],
        ).wait_recv()
        return x_r[side, step, q].astype(F32)

    def own(rel, q):
        return g_v[rel, :, q * piece : (q + 1) * piece]

    def rel_of(side, step):
        away = far - step
        return away if side == 0 else (nm - away) % nm

    def long_way(side, q):
        return (q < NQ // 2) == (side == 0)

    phase("products")
    product(far)
    for side in range(2):
        for q in range(NQ):
            if long_way(side, q):
                ring_send(side, 0, q, own(far, q))
    for side in range(2):
        product(rel_of(side, 1))
        for q in range(NQ):
            if not long_way(side, q):
                ring_send(side, 1, q, own(rel_of(side, 1), q))
    for step in range(2, far):
        for side in range(2):
            product(rel_of(side, step))
    product(0)

    phase("ring")
    w2x_sends = []
    for k in by_distance(nm):
        copy = remote(w2_own, w2_x.at[m], w2x_ss.at[k], w2x_rs.at[m], {"mp": lax.rem(m + k, nm)})
        copy.start()
        w2x_sends.append(copy)

    order = list(range(NQ))
    for q in order:
        for side in range(2):
            if long_way(side, q):
                ring_send(side, 1, q, ring_recv(side, 0, q) + own(rel_of(side, 1), q))
    for step in range(2, far):
        for q in order:
            for side in range(2):
                ring_send(side, step, q, ring_recv(side, step - 1, q) + own(rel_of(side, step), q))

    phase("w2_x")
    for k in by_distance(nm):
        src = lax.rem(m + k, nm)
        remote(w2_own, w2_x.at[src], w2x_ss.at[k], w2x_rs.at[src], {"mp": src}).wait_recv()
    w2_sum[0] = functools.reduce(lambda a, b: a + b, [w2_x[i] for i in range(nm)])
    w2_pair = remote(w2_sum.at[0], w2_in, pair_ss.at[2], pair_rs.at[2], {"sub": other})
    w2_pair.start()

    phase("ring_end")
    z_sends = []
    for q in order:
        block = own(0, q)
        for side in range(2):
            block = block + ring_recv(side, far - 1, q)
        z_s[q] = block.reshape(nd // 2, 16, piece).astype(BF16)
        z, par = q // 2, q % 2

        @pl.when(lax.rem(d, 2) == par)
        def _():
            z_r[z, d] = z_s[q, d // 2]

        for k in by_distance(nd):
            to = lax.rem(d + k, nd)
            copy = remote(z_s.at[q, to // 2], z_r.at[z, d], z_ss.at[z, k], z_rs.at[z, d], {"docs": to})
            z_sends.append((copy, to, par))
            pl.when(lax.rem(to, 2) == par)(copy.start)
        if q == 1:
            w2_pair.wait_recv()
            w2_sum[1] = w2_sum[0] + w2_in[...]
            w2_z[d] = w2_sum[1]
            w2z_sends = []
            for k in by_distance(nd):
                copy = remote(
                    w2_sum.at[1], w2_z.at[d], w2z_ss.at[k], w2z_rs.at[d], {"docs": lax.rem(d + k, nd)}
                )
                copy.start()
                w2z_sends.append(copy)

    phase("emb_grad")
    grad = lax.dot_general(
        pg[0], w1_v[:, :half], (((1,), (1,)), ((), ())), preferred_element_type=F32
    ) + lax.dot_general(pg[1], w1_v[:, half:], (((1,), (1,)), ((), ())), preferred_element_type=F32)
    eg_v[...] = grad.astype(BF16)
    phase("docs_sum")
    part = nd // 2
    core = d // part
    mine = lax.rem(d, part)
    ag_sends = []
    for z in range(2):
        for k in by_distance(nd):
            src = lax.rem(d + k, nd)
            remote(z_s.at[0, 0], z_r.at[z, src], z_ss.at[z, k], z_rs.at[z, src], {"docs": src}).wait_recv()
        z_f[z] = functools.reduce(lambda a, b: a + b, [z_r[z, i].astype(F32) for i in range(nd)]).astype(BF16)

        @pl.when(core == s)
        def _():
            ag_r[s, z, mine] = z_f[z]

        for k in by_distance(nd) + [0]:
            copy = remote(
                z_f.at[z], ag_r.at[s, z, mine], ag_ss.at[z, k], ag_rs.at[s, z, mine],
                {"docs": lax.rem(d + k, nd), "sub": core},
            )
            if k == 0:
                pl.when(core != s)(copy.start)
            else:
                copy.start()
            ag_sends.append((copy, k))

    phase("w2_z")
    for k in by_distance(nd):
        src = lax.rem(d + k, nd)
        remote(w2_sum.at[1], w2_z.at[src], w2z_ss.at[k], w2z_rs.at[src], {"docs": src}).wait_recv()
    w2_out[...] = functools.reduce(lambda a, b: a + b, [w2_z[i] for i in range(nd)])

    phase("docs_gather")
    for z in range(2):
        for src in range(2):
            for k in range(part):
                copy = remote(
                    z_f.at[z], ag_r.at[src, z, k], ag_ss.at[z, k], ag_rs.at[src, z, k], {"sub": other}
                )
                same = (src == s) & (s * part + k == d)
                pl.when(jnp.logical_not(same))(copy.wait_recv)
                out_v[(k // 2) * 16 : (k // 2) * 16 + 16, pl.ds(src * half + z * 256 + (k % 2) * 128, 128)] = ag_r[
                    src, z, k
                ].astype(F32)

    phase("drain")
    for copy in score_sends + meta_sends + [emb_send, pg_send, w2_pair] + x_sends + w2x_sends + w2z_sends:
        copy.wait_send()
    for copy, to, par in z_sends:
        pl.when(lax.rem(to, 2) == par)(copy.wait_send)
    for copy, k in ag_sends:
        if k == 0:
            pl.when(core != s)(copy.wait_send)
        else:
            copy.wait_send()
    phase(None)


def write_out(a, b, c, a_out, b_out, c_out, sem):
    copies = [pltpu.make_async_copy(x, y, sem.at[i]) for i, (x, y) in enumerate(((a, a_out), (b, b_out), (c, c_out)))]
    for copy in copies:
        copy.start()
    for copy in copies:
        copy.wait()


def solution(mesh):
    nd, nm = mesh.shape["docs"], mesh.shape["mp"]

    def on_device(embeddings, owner_shard, query_local, labels, w_first, w_second):
        rows, width = embeddings.shape
        cap = 2 * rows // nd
        slots = nd * cap
        half = width // 2
        piece = half // NQ
        far = nm // 2
        dma = pltpu.SemaphoreType.DMA
        hbm, vmem, anywhere = (pl.BlockSpec(memory_space=a) for a in (pltpu.HBM, pltpu.VMEM, pl.ANY))
        scratch = [
            pltpu.VMEM((rows, width), BF16),
            pltpu.VMEM((1, rows), jnp.int32),
            pltpu.VMEM((1, rows), jnp.int32),
            pltpu.VMEM((1, rows), jnp.int32),
            pltpu.VMEM((width, width), BF16),
            pltpu.VMEM((1, width), F32),
            pltpu.VMEM((rows, width), F32),
            pltpu.VMEM((rows, width), F32),
            pltpu.VMEM((rows, slots), F32),
            pltpu.VMEM((2, slots), BF16),
            pltpu.VMEM((nd, 2, slots), BF16),
            pltpu.VMEM((1, slots), F32),
            pltpu.VMEM((nd, 1, slots), F32),
            pltpu.VMEM((cap, nd, slots), F32),
            pltpu.VMEM((cap, nd, slots), F32),
            pltpu.VMEM((cap, nd, slots), F32),
            pltpu.VMEM((cap, nd, slots), F32),
            pltpu.VMEM((nd, slots), F32),
            pltpu.VMEM((rows, width), BF16),
            pltpu.VMEM((nm, width // nm, 2 * rows), BF16),
            pltpu.VMEM((2, rows, half), BF16),
            pltpu.VMEM((rows, half), BF16),
            pltpu.VMEM((nm, width // nm, half), F32),
            pltpu.VMEM((2, far, NQ, width // nm, piece), BF16),
            pltpu.VMEM((2, far, NQ, width // nm, piece), BF16),
            pltpu.VMEM((NQ, nd // 2, 16, piece), BF16),
            pltpu.VMEM((2, nd, 16, piece), BF16),
            pltpu.VMEM((2, 16, piece), BF16),
            pltpu.VMEM((2, 2, nd // 2, 16, piece), BF16),
            pltpu.VMEM((width // 128, 128), F32),
            pltpu.VMEM((nm, width // 128, 128), F32),
            pltpu.VMEM((2, width // 128, 128), F32),
            pltpu.VMEM((width // 128, 128), F32),
            pltpu.VMEM((nd, width // 128, 128), F32),
            dma((5 + FWD,)),
            dma((nd,)),
            dma((nd,)),
            dma((nd,)),
            dma((nd,)),
            dma((3,)),
            dma((3,)),
            dma((2, far, NQ)),
            dma((2, far, NQ)),
            dma((2, nd)),
            dma((2, nd)),
            dma((2, nd)),
            dma((2, 2, nd // 2)),
            dma((nm,)),
            dma((nm,)),
            dma((nd,)),
            dma((nd,)),
        ]
        shapes = (
            jax.ShapeDtypeStruct((rows, width), BF16),
            jax.ShapeDtypeStruct((width // nm // 2, width), F32),
            jax.ShapeDtypeStruct((width // 128, 128), F32),
        )
        results = pl.pallas_call(
            functools.partial(step_kernel, nd, nm, rows, width, cap),
            out_shape=tuple(pltpu.VMEM(a.shape, a.dtype) for a in shapes),
            in_specs=[hbm] * 6,
            out_specs=(vmem,) * 3,
            scratch_shapes=scratch,
            compiler_params=pltpu.CompilerParams(
                collective_id=0, has_side_effects=True, vmem_limit_bytes=40 * 1024 * 1024
            ),
            name="ranking_step",
        )(
            *(
                pltpu.with_memory_space_constraint(a, pltpu.HBM)
                for a in (
                    embeddings,
                    owner_shard.reshape(1, rows),
                    query_local.reshape(1, rows),
                    labels.reshape(1, rows),
                    w_first,
                    w_second.reshape(1, width),
                )
            )
        )
        emb_grad, w_first_grad, w_second_grad = pl.pallas_call(
            write_out,
            out_shape=shapes,
            in_specs=[anywhere] * 3,
            out_specs=(hbm,) * 3,
            scratch_shapes=[dma((3,))],
            compiler_params=pltpu.CompilerParams(vmem_limit_bytes=1024 * 1024),
            name="write_out",
        )(*results)
        return emb_grad, w_first_grad, w_second_grad.reshape(width)

    whole = ("groups", "docs", "mp", "sub")
    return jax.shard_map(
        on_device,
        mesh=mesh,
        in_specs=(P(whole, None), P(whole, None), P(whole), P(whole), P(), P()),
        out_specs=(P(whole, None), P(("groups", "mp", "sub"), None), P("groups")),
        check_vma=False,
    )
```

```python
import functools
import math

import jax
import jax.numpy as jnp
from jax import lax
from jax.experimental import pallas as pl
from jax.experimental.pallas import tpu as pltpu
from jax.sharding import PartitionSpec as P

MESH = pl.DeviceIdType.MESH
F32 = jnp.float32
BF16 = jnp.bfloat16

NQ = 4
LN2 = math.log(2.0)
FWD = 4


def remote(src, dst, send_sem, recv_sem, where):
    return pltpu.make_async_remote_copy(
        src_ref=src, dst_ref=dst, send_sem=send_sem, recv_sem=recv_sem, device_id=where, device_id_type=MESH
    )


class Phases:
    def __init__(self):
        self.scope = None

    def __call__(self, name):
        if self.scope is not None:
            self.scope.__exit__(None, None, None)
        self.scope = jax.named_scope(name) if name else None
        if self.scope is not None:
            self.scope.__enter__()


def by_distance(count):
    return sorted(range(1, count), key=lambda k: -min(k, count - k))


def step_kernel(
    nd, nm, rows, width, cap,
    emb_h, own_h, qry_h, lab_h, w1_h, w2_h,
    eg_v, out_v, w2_out,
    emb_v, own_v, qry_v, lab_v, w1_v, w2_v,
    slope_v, hid_v, hit_v,
    meta_s, meta_r, score_s, score_r,
    sa, sm, sg, sd,
    embp_v, emb_t, pg, pg_in, g_v,
    x_s, x_r, z_s, z_r, z_f, ag_r,
    w2_own, w2_x, w2_sum, w2_in, w2_z,
    load_sem, meta_ss, meta_rs, score_ss, score_rs,
    pair_ss, pair_rs, x_ss, x_rs, z_ss, z_rs, ag_ss, ag_rs,
    w2x_ss, w2x_rs, w2z_ss, w2z_rs,
):
    d = lax.axis_index("docs")
    m = lax.axis_index("mp")
    s = lax.axis_index("sub")
    other = 1 - s
    slots = nd * cap
    half = width // 2
    piece = half // NQ

    phase = Phases()
    phase("greet")
    loads = [
        pltpu.make_async_copy(a, b, load_sem.at[i])
        for i, (a, b) in enumerate(
            ((own_h, own_v), (qry_h, qry_v), (lab_h, lab_v), (w2_h, w2_v), (emb_h, emb_v))
        )
    ]
    cols = width // FWD
    w_loads = [
        pltpu.make_async_copy(
            w1_h.at[:, pl.ds(i * cols, cols)], w1_v.at[:, pl.ds(i * cols, cols)], load_sem.at[5 + i]
        )
        for i in range(FWD)
    ]
    for copy in loads + w_loads:
        copy.start()

    reach = nd // 4
    barrier = pltpu.get_barrier_semaphore()
    near = [k for k in by_distance(nd) if min(k, nd - k) <= reach]
    for k in near:
        pl.semaphore_signal(barrier, inc=1, device_id={"docs": lax.rem(d + k, nd)}, device_id_type=MESH)
    for k in (1, nm - 1):
        pl.semaphore_signal(barrier, inc=1, device_id={"mp": lax.rem(m + k, nm)}, device_id_type=MESH)
    pl.semaphore_signal(barrier, inc=1, device_id={"sub": other}, device_id_type=MESH)

    phase("own_slots")
    for copy in loads[:3]:
        copy.wait()
    row_i = lax.broadcasted_iota(jnp.int32, (rows, rows), 0)
    col_i = lax.broadcasted_iota(jnp.int32, (rows, rows), 1)
    eye = row_i == col_i

    def upright(row):
        return jnp.sum(jnp.where(eye, row, 0.0), axis=1, keepdims=True)

    own_row = own_v[...].astype(F32)
    own_col = upright(own_row)
    earlier = jnp.sum(
        jnp.where((own_col == own_row) & (col_i < row_i), 1.0, 0.0), axis=1, keepdims=True
    )
    slot_col = own_col * cap + earlier
    hit = slot_col == lax.broadcasted_iota(jnp.int32, (rows, slots), 1).astype(F32)
    hit_v[...] = jnp.where(hit, 1.0, 0.0)

    def slotted(col):
        return jnp.sum(jnp.where(hit_v[...] > 0.0, col, 0.0), axis=0, keepdims=True)

    mark_own = slotted(upright(qry_v[...].astype(F32)) + 1.0)
    label_own = slotted(upright(lab_v[...].astype(F32)))
    meta_s[0:1, :] = mark_own.astype(BF16)
    meta_s[1:2, :] = label_own.astype(BF16)
    meta_r[0, 0:1, :] = mark_own.astype(BF16)
    meta_r[0, 1:2, :] = label_own.astype(BF16)

    def to_near(src, dst, send_sem, recv_sem):
        copies = []
        for k in near:
            copies.append(remote(src, dst.at[nd - k], send_sem.at[k], recv_sem.at[nd - k], {"docs": lax.rem(d + k, nd)}))
            copies[-1].start()
        return copies

    def from_near(src, dst, send_sem, recv_sem):
        for k in near:
            remote(src, dst.at[k], send_sem.at[k], recv_sem.at[k], {"docs": lax.rem(d + k, nd)}).wait_recv()

    def relays(dst, send_sem, recv_sem):
        ahead, behind = {"docs": lax.rem(d + reach, nd)}, {"docs": lax.rem(d + nd - reach, nd)}
        return [
            remote(
                dst.at[pl.ds(nd - reach, reach)], dst.at[pl.ds(nd - 2 * reach, reach)],
                send_sem.at[nd - 2 * reach], recv_sem.at[nd - 2 * reach], ahead,
            ),
            remote(
                dst.at[pl.ds(1, reach - 1)], dst.at[pl.ds(reach + 1, reach - 1)],
                send_sem.at[reach + 1], recv_sem.at[reach + 1], behind,
            ),
        ]


    phase("barrier")
    pl.semaphore_wait(barrier, len(near) + 3)
    meta_sends = to_near(meta_s, meta_r, meta_ss, meta_rs)
    phase("scorer")
    for copy in loads[3:]:
        copy.wait()
    emb_send = remote(emb_v, embp_v, pair_ss.at[0], pair_rs.at[0], {"sub": other})
    emb_send.start()
    score = jnp.zeros((rows, 1), F32)
    for i in range(FWD):
        w_loads[i].wait()
        at = pl.ds(i * cols, cols)
        pre = jnp.dot(emb_v[...], w1_v[:, at], preferred_element_type=F32)
        sig = 0.5 + 0.5 * jnp.tanh(0.5 * pre)
        hid = pre * sig
        w2 = w2_v[:, at]
        hid_v[:, at] = hid
        score += jnp.sum(hid * w2, axis=1, keepdims=True)
        slope_v[:, at] = w2 * (sig * (1.0 + pre * (1.0 - sig)))
    score_own = slotted(0.5 * score)
    score_s[...] = score_own
    score_r[0] = score_own
    phase("send_scores")
    score_sends = to_near(score_s, score_r, score_ss, score_rs)
    from_near(meta_s, meta_r, meta_ss, meta_rs)
    meta_relays = relays(meta_r, meta_ss, meta_rs)
    for copy in meta_relays:
        copy.start()
    phase("turn")
    def turn(block, at):
        for c in range(nm):
            w = width // nm
            emb_t[c, :, at * rows : (at + 1) * rows] = (
                block[:, c * w : (c + 1) * w].astype(F32).T.astype(BF16)
            )

    turn(emb_v, 0)
    emb_send.wait_recv()
    turn(embp_v, 1)

    phase("near_wait")
    from_near(score_s, score_r, score_ss, score_rs)
    score_relays = relays(score_r, score_ss, score_rs)
    for copy in score_relays:
        copy.start()

    phase("meta_wait")
    for copy in meta_relays:
        copy.wait_recv()
    phase("meta_work")
    lane = lax.broadcasted_iota(jnp.int32, (nd, slots), 1)
    in_group = lax.rem(lane, cap)

    def turned(a, by):
        near = pltpu.roll(a, by, 1)
        far = pltpu.roll(a, by + slots - cap, 1)
        return jnp.where(in_group >= by, near, far)

    mark = jnp.concatenate([meta_r[i, 0:1, :].astype(F32) for i in range(nd)], axis=0)
    label = jnp.concatenate([meta_r[i, 1:2, :].astype(F32) for i in range(nd)], axis=0)
    gain = jnp.exp2(label) - 1.0
    sm[0] = mark
    sg[0] = gain

    for by in range(1, cap):
        sm[by] = turned(mark, by)
        sg[by] = turned(gain, by)

    group_r = lax.broadcasted_iota(jnp.int32, (slots, slots), 0) // cap
    group_c = lax.broadcasted_iota(jnp.int32, (slots, slots), 1) // cap
    groups = jnp.where(group_r == group_c, 1.0, 0.0).astype(BF16)
    tallies = []
    for q in (1.0, 2.0):
        for least in range(5):
            tallies.append(
                jnp.sum(jnp.where((mark == q) & (label >= float(least)), 1.0, 0.0), axis=0, keepdims=True)
            )
    tallies += [jnp.zeros((6, slots), F32)]
    counts = jnp.dot(jnp.concatenate(tallies, axis=0).astype(BF16), groups, preferred_element_type=F32)
    total = jnp.where(mark == 1.0, counts[0:1], counts[5:6])
    at_least = jnp.where(mark_own == 1.0, counts[1:5], counts[6:10])

    def rank_weight(r, acc):
        r = r.astype(F32)
        w = LN2 / jnp.log(jnp.full((4, slots), 2.0, F32) + r)
        return acc + jnp.where(at_least > r, w, 0.0)

    ladder = lax.fori_loop(0, slots, rank_weight, jnp.zeros((4, slots), F32), unroll=8)
    idcg = ladder[0:1] + 2.0 * ladder[1:2] + 4.0 * ladder[2:3] + 8.0 * ladder[3:4]
    inv = jnp.where(idcg > 0.0, 1.0 / jnp.where(idcg > 0.0, idcg, 1.0), 0.0)
    gain_own = jnp.exp2(label_own) - 1.0

    phase("score_wait")
    for copy in score_relays:
        copy.wait_recv()
    phase("soft_rank")
    scores = jnp.concatenate([score_r[i] for i in range(nd)], axis=0)
    sa[0] = scores
    for by in range(1, cap):
        sa[by] = turned(scores, by)

    def soft(by, acc):
        for j in range(nd):
            t = jnp.tanh(sa[by, j : j + 1, :] - scores)
            acc += jnp.where(sm[by, j : j + 1, :] == mark, t, 0.0)
        return acc

    acc = lax.fori_loop(0, cap, soft, jnp.zeros((nd, slots), F32))
    rank = jnp.where(mark > 0.0, 0.5 * (total - 1.0 + acc), 0.0)
    disc = LN2 / jnp.log(2.0 + rank)
    disc_own = disc[0:1, :]
    sd[0] = disc
    for by in range(1, cap):
        sd[by] = turned(disc, by)

    phase("lambdas")
    def pairs(by, acc):
        t = jnp.tanh(sa[by] - score_own)
        gap = sg[by] - gain_own
        term = jnp.abs(sd[by] - disc_own) * (gap - jnp.abs(gap) * t)
        return acc + jnp.where(sm[by] == mark_own, term, 0.0)

    acc = lax.fori_loop(0, cap, pairs, jnp.zeros((nd, slots), F32), unroll=2)
    lam_row = 0.5 * inv * jnp.sum(acc, axis=0, keepdims=True)
    lam = jnp.sum(jnp.where(hit_v[...] > 0.0, lam_row, 0.0), axis=1, keepdims=True)

    phase("pre_grad")
    for h in range(2):
        pg[h] = (lam * slope_v[:, h * half : (h + 1) * half]).astype(BF16)
    pg_send = remote(pg.at[other], pg_in, pair_ss.at[1], pair_rs.at[1], {"sub": other})
    pg_send.start()
    for i in range(width // 128):
        w2_own[i : i + 1, :] = jnp.sum(lam * hid_v[:, i * 128 : (i + 1) * 128], axis=0, keepdims=True)
    w2_x[m] = w2_own[...]
    phase("pair_wait")
    pg_send.wait_recv()
    both = jnp.concatenate([pg[s], pg_in[...]], axis=0)

    right, left = {"mp": lax.rem(m + 1, nm)}, {"mp": lax.rem(m + nm - 1, nm)}
    far = nm // 2

    def product(rel):
        g_v[rel] = jnp.dot(emb_t[lax.rem(m + rel, nm)], both, preferred_element_type=F32)

    x_sends = []

    def ring_send(side, step, q, value):
        x_s[side, step, q] = value.astype(BF16)
        copy = remote(
            x_s.at[side, step, q], x_r.at[side, step, q], x_ss.at[side, step, q], x_rs.at[side, step, q],
            (right, left)[side],
        )
        copy.start()
        x_sends.append(copy)

    def ring_recv(side, step, q):
        remote(
            x_s.at[side, step, q], x_r.at[side, step, q], x_ss.at[side, step, q], x_rs.at[side, step, q],
            (right, left)[side],
        ).wait_recv()
        return x_r[side, step, q].astype(F32)

    def own(rel, q):
        return g_v[rel, :, q * piece : (q + 1) * piece]

    def rel_of(side, step):
        away = far - step
        return away if side == 0 else (nm - away) % nm

    def long_way(side, q):
        return (q < NQ // 2) == (side == 0)

    phase("products")
    product(far)
    for side in range(2):
        for q in range(NQ):
            if long_way(side, q):
                ring_send(side, 0, q, own(far, q))
    for side in range(2):
        product(rel_of(side, 1))
        for q in range(NQ):
            if not long_way(side, q):
                ring_send(side, 1, q, own(rel_of(side, 1), q))
    for step in range(2, far):
        for side in range(2):
            product(rel_of(side, step))
    product(0)

    phase("ring")
    order = list(range(NQ))
    for q in order:
        for side in range(2):
            if long_way(side, q):
                ring_send(side, 1, q, ring_recv(side, 0, q) + own(rel_of(side, 1), q))
    for step in range(2, far):
        for q in order:
            for side in range(2):
                ring_send(side, step, q, ring_recv(side, step - 1, q) + own(rel_of(side, step), q))

    phase("ring_end")
    z_sends = []
    for q in order:
        block = own(0, q)
        for side in range(2):
            block = block + ring_recv(side, far - 1, q)
        z_s[q] = block.reshape(nd // 2, 16, piece).astype(BF16)
        z, par = q // 2, q % 2

        @pl.when(lax.rem(d, 2) == par)
        def _():
            z_r[z, d] = z_s[q, d // 2]

        for k in by_distance(nd):
            to = lax.rem(d + k, nd)
            copy = remote(z_s.at[q, to // 2], z_r.at[z, d], z_ss.at[z, k], z_rs.at[z, d], {"docs": to})
            z_sends.append((copy, to, par))
            pl.when(lax.rem(to, 2) == par)(copy.start)

    w2x_sends = []
    for k in by_distance(nm):
        copy = remote(w2_own, w2_x.at[m], w2x_ss.at[k], w2x_rs.at[m], {"mp": lax.rem(m + k, nm)})
        copy.start()
        w2x_sends.append(copy)

    phase("emb_grad")
    grad = lax.dot_general(
        pg[0], w1_v[:, :half], (((1,), (1,)), ((), ())), preferred_element_type=F32
    ) + lax.dot_general(pg[1], w1_v[:, half:], (((1,), (1,)), ((), ())), preferred_element_type=F32)
    eg_v[...] = grad.astype(BF16)
    phase("docs_sum")
    for k in by_distance(nm):
        src = lax.rem(m + k, nm)
        remote(w2_own, w2_x.at[src], w2x_ss.at[k], w2x_rs.at[src], {"mp": src}).wait_recv()
    w2_sum[0] = functools.reduce(lambda a, b: a + b, [w2_x[i] for i in range(nm)])
    w2_pair = remote(w2_sum.at[0], w2_in, pair_ss.at[2], pair_rs.at[2], {"sub": other})
    w2_pair.start()

    part = nd // 2
    core = d // part
    mine = lax.rem(d, part)
    ag_sends = []
    for z in range(2):
        for k in by_distance(nd):
            src = lax.rem(d + k, nd)
            remote(z_s.at[0, 0], z_r.at[z, src], z_ss.at[z, k], z_rs.at[z, src], {"docs": src}).wait_recv()
        z_f[z] = functools.reduce(lambda a, b: a + b, [z_r[z, i].astype(F32) for i in range(nd)]).astype(BF16)

        @pl.when(core == s)
        def _():
            ag_r[s, z, mine] = z_f[z]

        for k in by_distance(nd) + [0]:
            copy = remote(
                z_f.at[z], ag_r.at[s, z, mine], ag_ss.at[z, k], ag_rs.at[s, z, mine],
                {"docs": lax.rem(d + k, nd), "sub": core},
            )
            if k == 0:
                pl.when(core != s)(copy.start)
            else:
                copy.start()
            ag_sends.append((copy, k))
        if z == 0:
            w2_pair.wait_recv()
            w2_sum[1] = w2_sum[0] + w2_in[...]
            w2_z[d] = w2_sum[1]
            w2z_sends = []
            for k in by_distance(nd):
                copy = remote(
                    w2_sum.at[1], w2_z.at[d], w2z_ss.at[k], w2z_rs.at[d], {"docs": lax.rem(d + k, nd)}
                )
                copy.start()
                w2z_sends.append(copy)

    phase("w2_z")
    for k in by_distance(nd):
        src = lax.rem(d + k, nd)
        remote(w2_sum.at[1], w2_z.at[src], w2z_ss.at[k], w2z_rs.at[src], {"docs": src}).wait_recv()
    w2_out[...] = functools.reduce(lambda a, b: a + b, [w2_z[i] for i in range(nd)])

    phase("docs_gather")
    for z in range(2):
        for src in range(2):
            for k in range(part):
                copy = remote(
                    z_f.at[z], ag_r.at[src, z, k], ag_ss.at[z, k], ag_rs.at[src, z, k], {"sub": other}
                )
                same = (src == s) & (s * part + k == d)
                pl.when(jnp.logical_not(same))(copy.wait_recv)
                out_v[(k // 2) * 16 : (k // 2) * 16 + 16, pl.ds(src * half + z * 256 + (k % 2) * 128, 128)] = ag_r[
                    src, z, k
                ].astype(F32)

    phase("drain")
    for copy in score_sends + meta_sends + score_relays + meta_relays + [emb_send, pg_send, w2_pair] + x_sends + w2x_sends + w2z_sends:
        copy.wait_send()
    for copy, to, par in z_sends:
        pl.when(lax.rem(to, 2) == par)(copy.wait_send)
    for copy, k in ag_sends:
        if k == 0:
            pl.when(core != s)(copy.wait_send)
        else:
            copy.wait_send()
    phase(None)


def write_out(a, b, c, a_out, b_out, c_out, sem):
    copies = [pltpu.make_async_copy(x, y, sem.at[i]) for i, (x, y) in enumerate(((a, a_out), (b, b_out), (c, c_out)))]
    for copy in copies:
        copy.start()
    for copy in copies:
        copy.wait()


def solution(mesh):
    nd, nm = mesh.shape["docs"], mesh.shape["mp"]

    def on_device(embeddings, owner_shard, query_local, labels, w_first, w_second):
        rows, width = embeddings.shape
        cap = 2 * rows // nd
        slots = nd * cap
        half = width // 2
        piece = half // NQ
        far = nm // 2
        dma = pltpu.SemaphoreType.DMA
        hbm, vmem, anywhere = (pl.BlockSpec(memory_space=a) for a in (pltpu.HBM, pltpu.VMEM, pl.ANY))
        scratch = [
            pltpu.VMEM((rows, width), BF16),
            pltpu.VMEM((1, rows), jnp.int32),
            pltpu.VMEM((1, rows), jnp.int32),
            pltpu.VMEM((1, rows), jnp.int32),
            pltpu.VMEM((width, width), BF16),
            pltpu.VMEM((1, width), F32),
            pltpu.VMEM((rows, width), F32),
            pltpu.VMEM((rows, width), F32),
            pltpu.VMEM((rows, slots), F32),
            pltpu.VMEM((2, slots), BF16),
            pltpu.VMEM((nd, 2, slots), BF16),
            pltpu.VMEM((1, slots), F32),
            pltpu.VMEM((nd, 1, slots), F32),
            pltpu.VMEM((cap, nd, slots), F32),
            pltpu.VMEM((cap, nd, slots), F32),
            pltpu.VMEM((cap, nd, slots), F32),
            pltpu.VMEM((cap, nd, slots), F32),
            pltpu.VMEM((rows, width), BF16),
            pltpu.VMEM((nm, width // nm, 2 * rows), BF16),
            pltpu.VMEM((2, rows, half), BF16),
            pltpu.VMEM((rows, half), BF16),
            pltpu.VMEM((nm, width // nm, half), F32),
            pltpu.VMEM((2, far, NQ, width // nm, piece), BF16),
            pltpu.VMEM((2, far, NQ, width // nm, piece), BF16),
            pltpu.VMEM((NQ, nd // 2, 16, piece), BF16),
            pltpu.VMEM((2, nd, 16, piece), BF16),
            pltpu.VMEM((2, 16, piece), BF16),
            pltpu.VMEM((2, 2, nd // 2, 16, piece), BF16),
            pltpu.VMEM((width // 128, 128), F32),
            pltpu.VMEM((nm, width // 128, 128), F32),
            pltpu.VMEM((2, width // 128, 128), F32),
            pltpu.VMEM((width // 128, 128), F32),
            pltpu.VMEM((nd, width // 128, 128), F32),
            dma((5 + FWD,)),
            dma((nd,)),
            dma((nd,)),
            dma((nd,)),
            dma((nd,)),
            dma((3,)),
            dma((3,)),
            dma((2, far, NQ)),
            dma((2, far, NQ)),
            dma((2, nd)),
            dma((2, nd)),
            dma((2, nd)),
            dma((2, 2, nd // 2)),
            dma((nm,)),
            dma((nm,)),
            dma((nd,)),
            dma((nd,)),
        ]
        shapes = (
            jax.ShapeDtypeStruct((rows, width), BF16),
            jax.ShapeDtypeStruct((width // nm // 2, width), F32),
            jax.ShapeDtypeStruct((width // 128, 128), F32),
        )
        results = pl.pallas_call(
            functools.partial(step_kernel, nd, nm, rows, width, cap),
            out_shape=tuple(pltpu.VMEM(a.shape, a.dtype) for a in shapes),
            in_specs=[hbm] * 6,
            out_specs=(vmem,) * 3,
            scratch_shapes=scratch,
            compiler_params=pltpu.CompilerParams(
                collective_id=0, has_side_effects=True, vmem_limit_bytes=40 * 1024 * 1024
            ),
            name="ranking_step",
        )(
            *(
                pltpu.with_memory_space_constraint(a, pltpu.HBM)
                for a in (
                    embeddings,
                    owner_shard.reshape(1, rows),
                    query_local.reshape(1, rows),
                    labels.reshape(1, rows),
                    w_first,
                    w_second.reshape(1, width),
                )
            )
        )
        emb_grad, w_first_grad, w_second_grad = pl.pallas_call(
            write_out,
            out_shape=shapes,
            in_specs=[anywhere] * 3,
            out_specs=(hbm,) * 3,
            scratch_shapes=[dma((3,))],
            compiler_params=pltpu.CompilerParams(vmem_limit_bytes=1024 * 1024),
            name="write_out",
        )(*results)
        return emb_grad, w_first_grad, w_second_grad.reshape(width)

    whole = ("groups", "docs", "mp", "sub")
    return jax.shard_map(
        on_device,
        mesh=mesh,
        in_specs=(P(whole, None), P(whole, None), P(whole), P(whole), P(), P()),
        out_specs=(P(whole, None), P(("groups", "mp", "sub"), None), P("groups")),
        check_vma=False,
    )
```

```python
import functools
import math

import jax
import jax.numpy as jnp
from jax import lax
from jax.experimental import pallas as pl
from jax.experimental.pallas import tpu as pltpu
from jax.sharding import PartitionSpec as P

MESH = pl.DeviceIdType.MESH
F32 = jnp.float32
BF16 = jnp.bfloat16

NQ = 4
LN2 = math.log(2.0)
FWD = 4


def remote(src, dst, send_sem, recv_sem, where):
    return pltpu.make_async_remote_copy(
        src_ref=src, dst_ref=dst, send_sem=send_sem, recv_sem=recv_sem, device_id=where, device_id_type=MESH
    )


class Phases:
    def __init__(self):
        self.scope = None

    def __call__(self, name):
        if self.scope is not None:
            self.scope.__exit__(None, None, None)
        self.scope = jax.named_scope(name) if name else None
        if self.scope is not None:
            self.scope.__enter__()


def by_distance(count):
    return sorted(range(1, count), key=lambda k: -min(k, count - k))


def step_kernel(
    nd, nm, rows, width, cap,
    emb_h, own_h, qry_h, lab_h, w1_h, w2_h,
    eg_v, out_v, w2_out,
    emb_v, own_v, qry_v, lab_v, w1_v, w2_v,
    slope_v, hid_v, hit_v,
    meta_s, meta_r, score_s, score_r,
    sa, sm, sg, sd,
    embp_v, emb_t, pg, pg_in, g_v,
    x_s, x_r, z_s, z_r, z_f, ag_r,
    w2_own, w2_x, w2_sum, w2_in, w2_z,
    load_sem, meta_ss, meta_rs, score_ss, score_rs,
    pair_ss, pair_rs, x_ss, x_rs, z_ss, z_rs, ag_ss, ag_rs,
    w2x_ss, w2x_rs, w2z_ss, w2z_rs,
):
    d = lax.axis_index("docs")
    m = lax.axis_index("mp")
    s = lax.axis_index("sub")
    other = 1 - s
    slots = nd * cap
    half = width // 2
    piece = half // NQ

    phase = Phases()
    phase("greet")
    loads = [
        pltpu.make_async_copy(a, b, load_sem.at[i])
        for i, (a, b) in enumerate(
            ((own_h, own_v), (qry_h, qry_v), (lab_h, lab_v), (w2_h, w2_v), (emb_h, emb_v))
        )
    ]
    cols = width // FWD
    w_loads = [
        pltpu.make_async_copy(
            w1_h.at[:, pl.ds(i * cols, cols)], w1_v.at[:, pl.ds(i * cols, cols)], load_sem.at[5 + i]
        )
        for i in range(FWD)
    ]
    for copy in loads + w_loads:
        copy.start()

    reach = nd // 4
    barrier = pltpu.get_barrier_semaphore()
    near = [k for k in by_distance(nd) if min(k, nd - k) <= reach]
    for k in near:
        pl.semaphore_signal(barrier, inc=1, device_id={"docs": lax.rem(d + k, nd)}, device_id_type=MESH)
    for k in (1, nm - 1):
        pl.semaphore_signal(barrier, inc=1, device_id={"mp": lax.rem(m + k, nm)}, device_id_type=MESH)
    pl.semaphore_signal(barrier, inc=1, device_id={"sub": other}, device_id_type=MESH)

    phase("own_slots")
    for copy in loads[:3]:
        copy.wait()
    row_i = lax.broadcasted_iota(jnp.int32, (rows, rows), 0)
    col_i = lax.broadcasted_iota(jnp.int32, (rows, rows), 1)
    eye = row_i == col_i

    def upright(row):
        return jnp.sum(jnp.where(eye, row, 0.0), axis=1, keepdims=True)

    own_row = own_v[...].astype(F32)
    own_col = upright(own_row)
    earlier = jnp.sum(
        jnp.where((own_col == own_row) & (col_i < row_i), 1.0, 0.0), axis=1, keepdims=True
    )
    slot_col = own_col * cap + earlier
    hit = slot_col == lax.broadcasted_iota(jnp.int32, (rows, slots), 1).astype(F32)
    hit_v[...] = jnp.where(hit, 1.0, 0.0)

    def slotted(col):
        return jnp.sum(jnp.where(hit_v[...] > 0.0, col, 0.0), axis=0, keepdims=True)

    mark_own = slotted(upright(qry_v[...].astype(F32)) + 1.0)
    label_own = slotted(upright(lab_v[...].astype(F32)))
    meta_s[0:1, :] = mark_own.astype(BF16)
    meta_s[1:2, :] = label_own.astype(BF16)
    meta_r[0, 0:1, :] = mark_own.astype(BF16)
    meta_r[0, 1:2, :] = label_own.astype(BF16)

    def to_near(src, dst, send_sem, recv_sem):
        copies = []
        for k in near:
            copies.append(remote(src, dst.at[nd - k], send_sem.at[k], recv_sem.at[nd - k], {"docs": lax.rem(d + k, nd)}))
            copies[-1].start()
        return copies

    def from_near(src, dst, send_sem, recv_sem):
        for k in near:
            remote(src, dst.at[k], send_sem.at[k], recv_sem.at[k], {"docs": lax.rem(d + k, nd)}).wait_recv()

    def relays(dst, send_sem, recv_sem):
        ahead, behind = {"docs": lax.rem(d + reach, nd)}, {"docs": lax.rem(d + nd - reach, nd)}
        return [
            remote(
                dst.at[pl.ds(nd - reach, reach)], dst.at[pl.ds(nd - 2 * reach, reach)],
                send_sem.at[nd - 2 * reach], recv_sem.at[nd - 2 * reach], ahead,
            ),
            remote(
                dst.at[pl.ds(1, reach - 1)], dst.at[pl.ds(reach + 1, reach - 1)],
                send_sem.at[reach + 1], recv_sem.at[reach + 1], behind,
            ),
        ]


    phase("scorer")
    for copy in loads[3:]:
        copy.wait()
    score = jnp.zeros((rows, 1), F32)
    for i in range(FWD):
        w_loads[i].wait()
        at = pl.ds(i * cols, cols)
        pre = jnp.dot(emb_v[...], w1_v[:, at], preferred_element_type=F32)
        sig = 0.5 + 0.5 * jnp.tanh(0.5 * pre)
        hid = pre * sig
        w2 = w2_v[:, at]
        hid_v[:, at] = hid
        score += jnp.sum(hid * w2, axis=1, keepdims=True)
        slope_v[:, at] = w2 * (sig * (1.0 + pre * (1.0 - sig)))
    score_own = slotted(0.5 * score)
    score_s[...] = score_own
    score_r[0] = score_own
    phase("barrier")
    pl.semaphore_wait(barrier, len(near) + 3)
    phase("send_scores")
    meta_sends = to_near(meta_s, meta_r, meta_ss, meta_rs)
    score_sends = to_near(score_s, score_r, score_ss, score_rs)
    emb_send = remote(emb_v, embp_v, pair_ss.at[0], pair_rs.at[0], {"sub": other})
    emb_send.start()
    phase("near_meta")
    from_near(meta_s, meta_r, meta_ss, meta_rs)
    meta_relays = relays(meta_r, meta_ss, meta_rs)
    for copy in meta_relays:
        copy.start()
    phase("near_wait")
    from_near(score_s, score_r, score_ss, score_rs)
    score_relays = relays(score_r, score_ss, score_rs)
    for copy in score_relays:
        copy.start()

    phase("turn")
    def turn(block, at):
        for c in range(nm):
            w = width // nm
            emb_t[c, :, at * rows : (at + 1) * rows] = (
                block[:, c * w : (c + 1) * w].astype(F32).T.astype(BF16)
            )

    turn(emb_v, 0)
    emb_send.wait_recv()
    turn(embp_v, 1)

    phase("meta_wait")
    for copy in meta_relays:
        copy.wait_recv()
    phase("meta_work")
    lane = lax.broadcasted_iota(jnp.int32, (nd, slots), 1)
    in_group = lax.rem(lane, cap)

    def turned(a, by):
        near = pltpu.roll(a, by, 1)
        far = pltpu.roll(a, by + slots - cap, 1)
        return jnp.where(in_group >= by, near, far)

    mark = jnp.concatenate([meta_r[i, 0:1, :].astype(F32) for i in range(nd)], axis=0)
    label = jnp.concatenate([meta_r[i, 1:2, :].astype(F32) for i in range(nd)], axis=0)
    gain = jnp.exp2(label) - 1.0
    sm[0] = mark
    sg[0] = gain
    packed = 32.0 * mark + gain
    for by in range(1, cap):
        moved = turned(packed, by)
        moved_mark = jnp.floor(moved * (1.0 / 32.0))
        sm[by] = moved_mark
        sg[by] = moved - 32.0 * moved_mark

    group_r = lax.broadcasted_iota(jnp.int32, (slots, slots), 0) // cap
    group_c = lax.broadcasted_iota(jnp.int32, (slots, slots), 1) // cap
    groups = jnp.where(group_r == group_c, 1.0, 0.0).astype(BF16)
    tallies = []
    for q in (1.0, 2.0):
        for least in range(5):
            tallies.append(
                jnp.sum(jnp.where((mark == q) & (label >= float(least)), 1.0, 0.0), axis=0, keepdims=True)
            )
    tallies += [jnp.zeros((6, slots), F32)]
    counts = jnp.dot(jnp.concatenate(tallies, axis=0).astype(BF16), groups, preferred_element_type=F32)
    total = jnp.where(mark == 1.0, counts[0:1], counts[5:6])
    at_least = jnp.where(mark_own == 1.0, counts[1:5], counts[6:10])

    at_least = jnp.concatenate([at_least[:, : slots // 2], at_least[:, slots // 2 :]], axis=0)
    ladders = [jnp.zeros_like(at_least)] * 4
    for r in range(slots):
        ladders[r % 4] = ladders[r % 4] + jnp.where(at_least > float(r), 1.0 / math.log2(2.0 + r), 0.0)
    ladder = (ladders[0] + ladders[1]) + (ladders[2] + ladders[3])
    ladder = jnp.concatenate([ladder[:4], ladder[4:]], axis=1)
    idcg = ladder[0:1] + 2.0 * ladder[1:2] + 4.0 * ladder[2:3] + 8.0 * ladder[3:4]
    inv = jnp.where(idcg > 0.0, 1.0 / jnp.where(idcg > 0.0, idcg, 1.0), 0.0)
    gain_own = jnp.exp2(label_own) - 1.0

    phase("score_wait")
    for copy in score_relays:
        copy.wait_recv()
    phase("soft_rank")
    scores = jnp.concatenate([score_r[i] for i in range(nd)], axis=0)
    sa[0] = scores
    for by in range(1, cap):
        sa[by] = turned(scores, by)

    def soft(by, acc):
        for j in range(nd):
            t = jnp.tanh(sa[by, j : j + 1, :] - scores)
            acc += jnp.where(sm[by, j : j + 1, :] == mark, t, 0.0)
        return acc

    acc = lax.fori_loop(0, cap, soft, jnp.zeros((nd, slots), F32))
    rank = jnp.where(mark > 0.0, 0.5 * (total - 1.0 + acc), 0.0)
    disc = LN2 / jnp.log(2.0 + rank)
    disc_own = disc[0:1, :]
    sd[0] = disc
    for by in range(1, cap):
        sd[by] = turned(disc, by)

    phase("lambdas")
    def pairs(by, acc):
        t = jnp.tanh(sa[by] - score_own)
        gap = sg[by] - gain_own
        term = jnp.abs(sd[by] - disc_own) * (gap - jnp.abs(gap) * t)
        return acc + jnp.where(sm[by] == mark_own, term, 0.0)

    acc = lax.fori_loop(0, cap, pairs, jnp.zeros((nd, slots), F32), unroll=2)
    lam_row = 0.5 * inv * jnp.sum(acc, axis=0, keepdims=True)
    lam = jnp.sum(jnp.where(hit_v[...] > 0.0, lam_row, 0.0), axis=1, keepdims=True)

    phase("pre_grad")
    for h in range(2):
        pg[h] = (lam * slope_v[:, h * half : (h + 1) * half]).astype(BF16)
    pg_send = remote(pg.at[other], pg_in, pair_ss.at[1], pair_rs.at[1], {"sub": other})
    pg_send.start()
    for i in range(width // 128):
        w2_own[i : i + 1, :] = jnp.sum(lam * hid_v[:, i * 128 : (i + 1) * 128], axis=0, keepdims=True)
    w2_x[m] = w2_own[...]
    phase("pair_wait")
    pg_send.wait_recv()
    both = jnp.concatenate([pg[s], pg_in[...]], axis=0)

    right, left = {"mp": lax.rem(m + 1, nm)}, {"mp": lax.rem(m + nm - 1, nm)}
    far = nm // 2

    def product(rel):
        g_v[rel] = jnp.dot(emb_t[lax.rem(m + rel, nm)], both, preferred_element_type=F32)

    x_sends = []

    def ring_send(side, step, q, value):
        x_s[side, step, q] = value.astype(BF16)
        copy = remote(
            x_s.at[side, step, q], x_r.at[side, step, q], x_ss.at[side, step, q], x_rs.at[side, step, q],
            (right, left)[side],
        )
        copy.start()
        x_sends.append(copy)

    def ring_recv(side, step, q):
        remote(
            x_s.at[side, step, q], x_r.at[side, step, q], x_ss.at[side, step, q], x_rs.at[side, step, q],
            (right, left)[side],
        ).wait_recv()
        return x_r[side, step, q].astype(F32)

    def own(rel, q):
        return g_v[rel, :, q * piece : (q + 1) * piece]

    def rel_of(side, step):
        away = far - step
        return away if side == 0 else (nm - away) % nm

    def long_way(side, q):
        return (q < NQ // 2) == (side == 0)

    phase("products")
    product(far)
    for side in range(2):
        for q in range(NQ):
            if long_way(side, q):
                ring_send(side, 0, q, own(far, q))
    for side in range(2):
        product(rel_of(side, 1))
        for q in range(NQ):
            if not long_way(side, q):
                ring_send(side, 1, q, own(rel_of(side, 1), q))
    for step in range(2, far):
        for side in range(2):
            product(rel_of(side, step))
    product(0)

    phase("ring")
    longs = [[q for q in range(NQ) if long_way(side, q)] for side in range(2)]
    shorts = [[q for q in range(NQ) if not long_way(side, q)] for side in range(2)]

    def forward(step, pieces):
        for pair in zip(*pieces):
            for side, q in enumerate(pair):
                ring_send(side, step, q, ring_recv(side, step - 1, q) + own(rel_of(side, step), q))

    forward(1, longs)
    for step in range(2, far):
        forward(step, shorts)
        forward(step, longs)
    order = [q for pair in zip(*longs) for q in pair]

    phase("ring_end")
    z_sends = []
    for q in order:
        block = own(0, q)
        for side in range(2):
            block = block + ring_recv(side, far - 1, q)
        z_s[q] = block.reshape(nd // 2, 16, piece).astype(BF16)
        z, par = q // 2, q % 2

        @pl.when(lax.rem(d, 2) == par)
        def _():
            z_r[z, d] = z_s[q, d // 2]

        for k in by_distance(nd):
            to = lax.rem(d + k, nd)
            copy = remote(z_s.at[q, to // 2], z_r.at[z, d], z_ss.at[z, k], z_rs.at[z, d], {"docs": to})
            z_sends.append((copy, to, par))
            pl.when(lax.rem(to, 2) == par)(copy.start)

    w2x_sends = []
    for k in by_distance(nm):
        copy = remote(w2_own, w2_x.at[m], w2x_ss.at[k], w2x_rs.at[m], {"mp": lax.rem(m + k, nm)})
        copy.start()
        w2x_sends.append(copy)

    phase("emb_grad")
    grad = lax.dot_general(
        pg[0], w1_v[:, :half], (((1,), (1,)), ((), ())), preferred_element_type=F32
    ) + lax.dot_general(pg[1], w1_v[:, half:], (((1,), (1,)), ((), ())), preferred_element_type=F32)
    eg_v[...] = grad.astype(BF16)
    phase("docs_sum")
    for k in by_distance(nm):
        src = lax.rem(m + k, nm)
        remote(w2_own, w2_x.at[src], w2x_ss.at[k], w2x_rs.at[src], {"mp": src}).wait_recv()
    w2_sum[0] = functools.reduce(lambda a, b: a + b, [w2_x[i] for i in range(nm)])
    w2_pair = remote(w2_sum.at[0], w2_in, pair_ss.at[2], pair_rs.at[2], {"sub": other})
    w2_pair.start()

    part = nd // 2
    core = d // part
    mine = lax.rem(d, part)
    ag_sends = []
    for z in range(2):
        for k in by_distance(nd):
            src = lax.rem(d + k, nd)
            remote(z_s.at[0, 0], z_r.at[z, src], z_ss.at[z, k], z_rs.at[z, src], {"docs": src}).wait_recv()
        z_f[z] = functools.reduce(lambda a, b: a + b, [z_r[z, i].astype(F32) for i in range(nd)]).astype(BF16)

        @pl.when(core == s)
        def _():
            ag_r[s, z, mine] = z_f[z]

        for k in by_distance(nd) + [0]:
            copy = remote(
                z_f.at[z], ag_r.at[s, z, mine], ag_ss.at[z, k], ag_rs.at[s, z, mine],
                {"docs": lax.rem(d + k, nd), "sub": core},
            )
            if k == 0:
                pl.when(core != s)(copy.start)
            else:
                copy.start()
            ag_sends.append((copy, k))
        if z == 0:
            w2_pair.wait_recv()
            w2_sum[1] = w2_sum[0] + w2_in[...]
            w2_z[d] = w2_sum[1]
            w2z_sends = []
            for k in by_distance(nd):
                copy = remote(
                    w2_sum.at[1], w2_z.at[d], w2z_ss.at[k], w2z_rs.at[d], {"docs": lax.rem(d + k, nd)}
                )
                copy.start()
                w2z_sends.append(copy)

    phase("w2_z")
    for k in by_distance(nd):
        src = lax.rem(d + k, nd)
        remote(w2_sum.at[1], w2_z.at[src], w2z_ss.at[k], w2z_rs.at[src], {"docs": src}).wait_recv()
    w2_out[...] = functools.reduce(lambda a, b: a + b, [w2_z[i] for i in range(nd)])

    phase("docs_gather")
    for z in range(2):
        for src in range(2):
            for k in range(part):
                copy = remote(
                    z_f.at[z], ag_r.at[src, z, k], ag_ss.at[z, k], ag_rs.at[src, z, k], {"sub": other}
                )
                same = (src == s) & (s * part + k == d)
                pl.when(jnp.logical_not(same))(copy.wait_recv)
                out_v[(k // 2) * 16 : (k // 2) * 16 + 16, pl.ds(src * half + z * 256 + (k % 2) * 128, 128)] = ag_r[
                    src, z, k
                ].astype(F32)

    phase("drain")
    for copy in score_sends + meta_sends + score_relays + meta_relays + [emb_send, pg_send, w2_pair] + x_sends + w2x_sends + w2z_sends:
        copy.wait_send()
    for copy, to, par in z_sends:
        pl.when(lax.rem(to, 2) == par)(copy.wait_send)
    for copy, k in ag_sends:
        if k == 0:
            pl.when(core != s)(copy.wait_send)
        else:
            copy.wait_send()
    phase(None)


def write_out(a, b, c, a_out, b_out, c_out, sem):
    copies = [pltpu.make_async_copy(x, y, sem.at[i]) for i, (x, y) in enumerate(((a, a_out), (b, b_out), (c, c_out)))]
    for copy in copies:
        copy.start()
    for copy in copies:
        copy.wait()


def solution(mesh):
    nd, nm = mesh.shape["docs"], mesh.shape["mp"]

    def on_device(embeddings, owner_shard, query_local, labels, w_first, w_second):
        rows, width = embeddings.shape
        cap = 2 * rows // nd
        slots = nd * cap
        half = width // 2
        piece = half // NQ
        far = nm // 2
        dma = pltpu.SemaphoreType.DMA
        hbm, vmem, anywhere = (pl.BlockSpec(memory_space=a) for a in (pltpu.HBM, pltpu.VMEM, pl.ANY))
        scratch = [
            pltpu.VMEM((rows, width), BF16),
            pltpu.VMEM((1, rows), jnp.int32),
            pltpu.VMEM((1, rows), jnp.int32),
            pltpu.VMEM((1, rows), jnp.int32),
            pltpu.VMEM((width, width), BF16),
            pltpu.VMEM((1, width), F32),
            pltpu.VMEM((rows, width), F32),
            pltpu.VMEM((rows, width), F32),
            pltpu.VMEM((rows, slots), F32),
            pltpu.VMEM((2, slots), BF16),
            pltpu.VMEM((nd, 2, slots), BF16),
            pltpu.VMEM((1, slots), F32),
            pltpu.VMEM((nd, 1, slots), F32),
            pltpu.VMEM((cap, nd, slots), F32),
            pltpu.VMEM((cap, nd, slots), F32),
            pltpu.VMEM((cap, nd, slots), F32),
            pltpu.VMEM((cap, nd, slots), F32),
            pltpu.VMEM((rows, width), BF16),
            pltpu.VMEM((nm, width // nm, 2 * rows), BF16),
            pltpu.VMEM((2, rows, half), BF16),
            pltpu.VMEM((rows, half), BF16),
            pltpu.VMEM((nm, width // nm, half), F32),
            pltpu.VMEM((2, far, NQ, width // nm, piece), BF16),
            pltpu.VMEM((2, far, NQ, width // nm, piece), BF16),
            pltpu.VMEM((NQ, nd // 2, 16, piece), BF16),
            pltpu.VMEM((2, nd, 16, piece), BF16),
            pltpu.VMEM((2, 16, piece), BF16),
            pltpu.VMEM((2, 2, nd // 2, 16, piece), BF16),
            pltpu.VMEM((width // 128, 128), F32),
            pltpu.VMEM((nm, width // 128, 128), F32),
            pltpu.VMEM((2, width // 128, 128), F32),
            pltpu.VMEM((width // 128, 128), F32),
            pltpu.VMEM((nd, width // 128, 128), F32),
            dma((5 + FWD,)),
            dma((nd,)),
            dma((nd,)),
            dma((nd,)),
            dma((nd,)),
            dma((3,)),
            dma((3,)),
            dma((2, far, NQ)),
            dma((2, far, NQ)),
            dma((2, nd)),
            dma((2, nd)),
            dma((2, nd)),
            dma((2, 2, nd // 2)),
            dma((nm,)),
            dma((nm,)),
            dma((nd,)),
            dma((nd,)),
        ]
        shapes = (
            jax.ShapeDtypeStruct((rows, width), BF16),
            jax.ShapeDtypeStruct((width // nm // 2, width), F32),
            jax.ShapeDtypeStruct((width // 128, 128), F32),
        )
        results = pl.pallas_call(
            functools.partial(step_kernel, nd, nm, rows, width, cap),
            out_shape=tuple(pltpu.VMEM(a.shape, a.dtype) for a in shapes),
            in_specs=[hbm] * 6,
            out_specs=(vmem,) * 3,
            scratch_shapes=scratch,
            compiler_params=pltpu.CompilerParams(
                collective_id=0, has_side_effects=True, vmem_limit_bytes=40 * 1024 * 1024
            ),
            name="ranking_step",
        )(
            *(
                pltpu.with_memory_space_constraint(a, pltpu.HBM)
                for a in (
                    embeddings,
                    owner_shard.reshape(1, rows),
                    query_local.reshape(1, rows),
                    labels.reshape(1, rows),
                    w_first,
                    w_second.reshape(1, width),
                )
            )
        )
        emb_grad, w_first_grad, w_second_grad = pl.pallas_call(
            write_out,
            out_shape=shapes,
            in_specs=[anywhere] * 3,
            out_specs=(hbm,) * 3,
            scratch_shapes=[dma((3,))],
            compiler_params=pltpu.CompilerParams(vmem_limit_bytes=1024 * 1024),
            name="write_out",
        )(*results)
        return emb_grad, w_first_grad, w_second_grad.reshape(width)

    whole = ("groups", "docs", "mp", "sub")
    return jax.shard_map(
        on_device,
        mesh=mesh,
        in_specs=(P(whole, None), P(whole, None), P(whole), P(whole), P(), P()),
        out_specs=(P(whole, None), P(("groups", "mp", "sub"), None), P("groups")),
        check_vma=False,
    )
```

```python
import functools
import math

import jax
import jax.numpy as jnp
from jax import lax
from jax.experimental import pallas as pl
from jax.experimental.pallas import tpu as pltpu
from jax.sharding import PartitionSpec as P

MESH = pl.DeviceIdType.MESH
F32 = jnp.float32
BF16 = jnp.bfloat16

NQ = 4
LN2 = math.log(2.0)
NW = 4
EMB = 4


def remote(src, dst, send_sem, recv_sem, where):
    return pltpu.make_async_remote_copy(
        src_ref=src, dst_ref=dst, send_sem=send_sem, recv_sem=recv_sem, device_id=where, device_id_type=MESH
    )


class Phases:
    def __init__(self):
        self.scope = None

    def __call__(self, name):
        if self.scope is not None:
            self.scope.__exit__(None, None, None)
        self.scope = jax.named_scope(name) if name else None
        if self.scope is not None:
            self.scope.__enter__()


def by_distance(count):
    return sorted(range(1, count), key=lambda k: -min(k, count - k))


def step_kernel(
    nd, nm, rows, width, cap,
    emb_h, own_h, qry_h, lab_h, w1_h, w2_h,
    eg_v, out_v, w2_out,
    emb_v, own_v, qry_v, lab_v, w1_v, w2_v, w2_q,
    slope_v, hid_v, hit_v,
    meta_s, meta_r, score_s, score_r,
    sa, sm, sg, sd,
    emb_x, emb_t, pg, slope_x, lam_s, lam_r, g_v,
    x_s, x_r, z_s, z_r, z_f, ag_r,
    w2_own, w2_x, w2_sum, w2_in, w2_z,
    load_sem, meta_ss, meta_rs, score_ss, score_rs,
    pair_ss, pair_rs, emb_ss, emb_rs, lam_ss, lam_rs, x_ss, x_rs, z_ss, z_rs, ag_ss, ag_rs,
    w2x_ss, w2x_rs, w2z_ss, w2z_rs,
):
    d = lax.axis_index("docs")
    m = lax.axis_index("mp")
    s = lax.axis_index("sub")
    other = 1 - s
    slots = nd * cap
    quarter = width // NW
    block_rows = width // nm
    tiles = block_rows // 16
    par = lax.rem(d, 2)
    pair = d + 1 - 2 * par
    mine_q = 2 * s + par

    phase = Phases()
    phase("greet")
    loads = [
        pltpu.make_async_copy(a, b, load_sem.at[i])
        for i, (a, b) in enumerate(
            ((own_h, own_v), (qry_h, qry_v), (lab_h, lab_v), (w2_h, w2_v), (emb_h, emb_v))
        )
    ]
    w_loads = [
        pltpu.make_async_copy(w1_h.at[:, pl.ds(i * quarter, quarter)], w1_v.at[i], load_sem.at[5 + i])
        for i in range(NW)
    ]
    for copy in loads + w_loads:
        copy.start()

    reach = nd // 4
    barrier = pltpu.get_barrier_semaphore()
    near = [k for k in by_distance(nd) if min(k, nd - k) <= reach]
    for k in near:
        pl.semaphore_signal(barrier, inc=1, device_id={"docs": lax.rem(d + k, nd)}, device_id_type=MESH)
    for k in (1, nm - 1):
        pl.semaphore_signal(barrier, inc=1, device_id={"mp": lax.rem(m + k, nm)}, device_id_type=MESH)
    pl.semaphore_signal(barrier, inc=1, device_id={"sub": other}, device_id_type=MESH)
    pl.semaphore_signal(barrier, inc=1, device_id={"docs": pair, "sub": other}, device_id_type=MESH)

    phase("own_slots")
    for copy in loads[:3]:
        copy.wait()
    row_i = lax.broadcasted_iota(jnp.int32, (rows, rows), 0)
    col_i = lax.broadcasted_iota(jnp.int32, (rows, rows), 1)
    eye = row_i == col_i

    def upright(row):
        return jnp.sum(jnp.where(eye, row, 0.0), axis=1, keepdims=True)

    own_row = own_v[...].astype(F32)
    own_col = upright(own_row)
    earlier = jnp.sum(
        jnp.where((own_col == own_row) & (col_i < row_i), 1.0, 0.0), axis=1, keepdims=True
    )
    slot_col = own_col * cap + earlier
    hit = slot_col == lax.broadcasted_iota(jnp.int32, (rows, slots), 1).astype(F32)
    hit_v[...] = jnp.where(hit, 1.0, 0.0)

    def slotted(col):
        return jnp.sum(jnp.where(hit_v[...] > 0.0, col, 0.0), axis=0, keepdims=True)

    mark_own = slotted(upright(qry_v[...].astype(F32)) + 1.0)
    label_own = slotted(upright(lab_v[...].astype(F32)))
    meta_s[0:1, :] = mark_own.astype(BF16)
    meta_s[1:2, :] = label_own.astype(BF16)
    meta_r[0, 0:1, :] = mark_own.astype(BF16)
    meta_r[0, 1:2, :] = label_own.astype(BF16)

    def to_near(src, dst, send_sem, recv_sem):
        copies = []
        for k in near:
            copies.append(remote(src, dst.at[nd - k], send_sem.at[k], recv_sem.at[nd - k], {"docs": lax.rem(d + k, nd)}))
            copies[-1].start()
        return copies

    def from_near(src, dst, send_sem, recv_sem):
        for k in near:
            remote(src, dst.at[k], send_sem.at[k], recv_sem.at[k], {"docs": lax.rem(d + k, nd)}).wait_recv()

    def relays(dst, send_sem, recv_sem):
        ahead, behind = {"docs": lax.rem(d + reach, nd)}, {"docs": lax.rem(d + nd - reach, nd)}
        return [
            remote(
                dst.at[pl.ds(nd - reach, reach)], dst.at[pl.ds(nd - 2 * reach, reach)],
                send_sem.at[nd - 2 * reach], recv_sem.at[nd - 2 * reach], ahead,
            ),
            remote(
                dst.at[pl.ds(1, reach - 1)], dst.at[pl.ds(reach + 1, reach - 1)],
                send_sem.at[reach + 1], recv_sem.at[reach + 1], behind,
            ),
        ]


    phase("scorer")
    for copy in loads[3:] + w_loads:
        copy.wait()
    terms = jnp.zeros((rows, quarter), F32)
    for i in range(NW):
        at = pl.ds(i * quarter, quarter)
        pre = jnp.dot(emb_v[...], w1_v[i], preferred_element_type=F32)
        sig = 0.5 + 0.5 * jnp.tanh(0.5 * pre)
        hid = pre * sig
        hid_v[:, at] = hid
        slope_v[:, at] = sig
        w2_q[i] = w2_v[:, at]
        terms += hid * w2_v[:, at]
    score = jnp.sum(terms, axis=1, keepdims=True)
    score_own = slotted(0.5 * score)
    score_s[...] = score_own
    score_r[0] = score_own
    phase("barrier")
    pl.semaphore_wait(barrier, len(near) + 4)
    phase("send_scores")
    meta_sends = to_near(meta_s, meta_r, meta_ss, meta_rs)
    score_sends = to_near(score_s, score_r, score_ss, score_rs)
    emb_send = remote(emb_v, emb_x.at[0], pair_ss.at[0], pair_rs.at[0], {"sub": other})
    emb_send.start()
    share = rows // EMB
    emb_moves = [
        remote(
            emb_v.at[pl.ds(i * share, share)], emb_x.at[1, pl.ds(i * share, share)],
            emb_ss.at[i], emb_rs.at[i], {"docs": pair},
        )
        for i in range(EMB)
    ]
    for copy in emb_moves[:-1]:
        copy.start()
    phase("near_meta")
    from_near(meta_s, meta_r, meta_ss, meta_rs)
    meta_relays = relays(meta_r, meta_ss, meta_rs)
    for copy in meta_relays:
        copy.start()
    phase("near_wait")
    from_near(score_s, score_r, score_ss, score_rs)
    score_relays = relays(score_r, score_ss, score_rs)
    for copy in score_relays:
        copy.start()

    emb_moves[-1].start()

    phase("turn")
    def turn(block, at):
        for c in range(nm):
            emb_t[c, :, at * rows : (at + 1) * rows] = (
                block[:, c * block_rows : (c + 1) * block_rows].astype(F32).T.astype(BF16)
            )

    def slope_of(i):
        pre = jnp.dot(emb_x[i], w1_v[mine_q], preferred_element_type=F32)
        sig = 0.5 + 0.5 * jnp.tanh(0.5 * pre)
        slope_x[i] = w2_q[mine_q] * (sig + pre * sig * (1.0 - sig))

    turn(emb_v, 0)
    for i in range(NW):
        at = pl.ds(i * quarter, quarter)
        sig = slope_v[:, at]
        slope_v[:, at] = w2_v[:, at] * (sig + hid_v[:, at] * (1.0 - sig))
    emb_send.wait_recv()
    turn(emb_x.at[0], 1)
    slope_of(0)

    phase("meta_wait")
    for copy in meta_relays:
        copy.wait_recv()
    phase("emb_wait")
    for copy in emb_moves:
        copy.wait_recv()
    emb_pass = remote(emb_x.at[1], emb_x.at[2], pair_ss.at[1], pair_rs.at[1], {"sub": other})
    emb_pass.start()
    phase("meta_work")
    lane = lax.broadcasted_iota(jnp.int32, (nd, slots), 1)
    in_group = lax.rem(lane, cap)

    def turned(a, by):
        near = pltpu.roll(a, by, 1)
        far = pltpu.roll(a, by + slots - cap, 1)
        return jnp.where(in_group >= by, near, far)

    mark = jnp.concatenate([meta_r[i, 0:1, :].astype(F32) for i in range(nd)], axis=0)
    label = jnp.concatenate([meta_r[i, 1:2, :].astype(F32) for i in range(nd)], axis=0)
    gain = jnp.exp2(label) - 1.0
    sm[0] = mark
    sg[0] = gain
    packed = 32.0 * mark + gain
    for by in range(1, cap):
        moved = turned(packed, by)
        moved_mark = jnp.floor(moved * (1.0 / 32.0))
        sm[by] = moved_mark
        sg[by] = moved - 32.0 * moved_mark

    group_r = lax.broadcasted_iota(jnp.int32, (slots, slots), 0) // cap
    group_c = lax.broadcasted_iota(jnp.int32, (slots, slots), 1) // cap
    groups = jnp.where(group_r == group_c, 1.0, 0.0).astype(BF16)
    tallies = []
    for q in (1.0, 2.0):
        for least in range(5):
            tallies.append(
                jnp.sum(jnp.where((mark == q) & (label >= float(least)), 1.0, 0.0), axis=0, keepdims=True)
            )
    tallies += [jnp.zeros((6, slots), F32)]
    counts = jnp.dot(jnp.concatenate(tallies, axis=0).astype(BF16), groups, preferred_element_type=F32)
    total = jnp.where(mark == 1.0, counts[0:1], counts[5:6])
    at_least = jnp.where(mark_own == 1.0, counts[1:5], counts[6:10])

    at_least = jnp.concatenate([at_least[:, : slots // 2], at_least[:, slots // 2 :]], axis=0)
    ladders = [jnp.zeros_like(at_least)] * 4
    for r in range(slots):
        ladders[r % 4] = ladders[r % 4] + jnp.where(at_least > float(r), 1.0 / math.log2(2.0 + r), 0.0)
    ladder = (ladders[0] + ladders[1]) + (ladders[2] + ladders[3])
    ladder = jnp.concatenate([ladder[:4], ladder[4:]], axis=1)
    idcg = ladder[0:1] + 2.0 * ladder[1:2] + 4.0 * ladder[2:3] + 8.0 * ladder[3:4]
    inv = jnp.where(idcg > 0.0, 1.0 / jnp.where(idcg > 0.0, idcg, 1.0), 0.0)
    gain_own = jnp.exp2(label_own) - 1.0

    phase("score_wait")
    for copy in score_relays:
        copy.wait_recv()
    phase("soft_rank")
    scores = jnp.concatenate([score_r[i] for i in range(nd)], axis=0)
    sa[0] = scores
    for by in range(1, cap):
        sa[by] = turned(scores, by)

    def soft(by, acc):
        for j in range(nd):
            t = jnp.tanh(sa[by, j : j + 1, :] - scores)
            acc += jnp.where(sm[by, j : j + 1, :] == mark, t, 0.0)
        return acc

    acc = lax.fori_loop(0, cap, soft, jnp.zeros((nd, slots), F32))
    rank = jnp.where(mark > 0.0, 0.5 * (total - 1.0 + acc), 0.0)
    disc = LN2 / jnp.log(2.0 + rank)
    disc_own = disc[0:1, :]
    sd[0] = disc
    for by in range(1, cap):
        sd[by] = turned(disc, by)

    phase("lambdas")
    def pairs(by, acc):
        t = jnp.tanh(sa[by] - score_own)
        gap = sg[by] - gain_own
        term = jnp.abs(sd[by] - disc_own) * (gap - jnp.abs(gap) * t)
        return acc + jnp.where(sm[by] == mark_own, term, 0.0)

    acc = lax.fori_loop(0, cap, pairs, jnp.zeros((nd, slots), F32), unroll=2)
    lam_row = 0.5 * inv * jnp.sum(acc, axis=0, keepdims=True)
    lam = jnp.sum(jnp.where(hit_v[...] > 0.0, lam_row, 0.0), axis=1, keepdims=True)

    phase("pre_grad")
    lam_s[...] = jnp.sum(jnp.where(eye, lam, 0.0), axis=0, keepdims=True)
    quad = ({"sub": other}, {"docs": pair}, {"docs": pair, "sub": other})
    lam_sends = [remote(lam_s, lam_r.at[i], lam_ss.at[i], lam_rs.at[i], where) for i, where in enumerate(quad)]
    for copy in reversed(lam_sends):
        copy.start()
    for i in range(NW):
        pg[i] = (lam * slope_v[:, i * quarter : (i + 1) * quarter]).astype(BF16)
    turn(emb_x.at[1], 2)
    slope_of(1)
    for i in range(width // 128):
        w2_own[i : i + 1, :] = jnp.sum(lam * hid_v[:, i * 128 : (i + 1) * 128], axis=0, keepdims=True)
    w2_x[m] = w2_own[...]
    phase("emb_pass_wait")
    emb_pass.wait_recv()
    turn(emb_x.at[2], 3)
    slope_of(2)
    phase("pair_wait")
    for copy in lam_sends:
        copy.wait_recv()
    phase("products")
    both = jnp.concatenate(
        [pg[mine_q]] + [(upright(lam_r[i]) * slope_x[i]).astype(BF16) for i in range(3)], axis=0
    )

    right, left = {"mp": lax.rem(m + 1, nm)}, {"mp": lax.rem(m + nm - 1, nm)}
    far = nm // 2

    def product(rel):
        g_v[rel] = jnp.dot(emb_t[lax.rem(m + rel, nm)], both, preferred_element_type=F32)

    x_sends = []

    def ring_send(side, step, q, value):
        x_s[side, step, q] = value.astype(BF16)
        copy = remote(
            x_s.at[side, step, q], x_r.at[side, step, q], x_ss.at[side, step, q], x_rs.at[side, step, q],
            (right, left)[side],
        )
        copy.start()
        x_sends.append(copy)

    def ring_recv(side, step, q):
        remote(
            x_s.at[side, step, q], x_r.at[side, step, q], x_ss.at[side, step, q], x_rs.at[side, step, q],
            (right, left)[side],
        ).wait_recv()
        return x_r[side, step, q].astype(F32)

    def own(rel, q):
        lanes = slice((q % 2) * 128, (q % 2) * 128 + 128)
        return jnp.stack([g_v[rel, e * 16 : e * 16 + 16, lanes] for e in range(q // 2, tiles, 2)])

    def rel_of(side, step):
        away = far - step
        return away if side == 0 else (nm - away) % nm

    def long_way(side, q):
        return (q < NQ // 2) == (side == 0)

    product(far)
    for side in range(2):
        for q in range(NQ):
            if long_way(side, q):
                ring_send(side, 0, q, own(far, q))
    for side in range(2):
        product(rel_of(side, 1))
        for q in range(NQ):
            if not long_way(side, q):
                ring_send(side, 1, q, own(rel_of(side, 1), q))
    for step in range(2, far):
        for side in range(2):
            product(rel_of(side, step))
    product(0)

    phase("ring")
    longs = [[q for q in range(NQ) if long_way(side, q)] for side in range(2)]
    shorts = [[q for q in range(NQ) if not long_way(side, q)] for side in range(2)]

    def forward(step, pieces):
        for pair in zip(*pieces):
            for side, q in enumerate(pair):
                ring_send(side, step, q, ring_recv(side, step - 1, q) + own(rel_of(side, step), q))

    forward(1, longs)
    for step in range(2, far):
        forward(step, shorts)
        forward(step, longs)
    order = [q for pair in zip(*longs) for q in pair]

    phase("ring_end")
    z_sends = []
    planes = nd // 2
    plane = d // 2
    for q in order:
        block = own(0, q)
        for side in range(2):
            block = block + ring_recv(side, far - 1, q)
        z_s[q] = block.astype(BF16)
        group, z = q // 2, q % 2

        @pl.when(lax.rem(plane, 2) == group)
        def _():
            z_r[z, plane] = z_s[q, plane // 2]

        for k in by_distance(planes):
            to = lax.rem(plane + k, planes)
            copy = remote(
                z_s.at[q, to // 2], z_r.at[z, plane], z_ss.at[z, k], z_rs.at[z, plane], {"docs": 2 * to + par}
            )
            z_sends.append((copy, to, group))
            pl.when(lax.rem(to, 2) == group)(copy.start)

    w2x_sends = []
    for k in by_distance(nm):
        copy = remote(w2_own, w2_x.at[m], w2x_ss.at[k], w2x_rs.at[m], {"mp": lax.rem(m + k, nm)})
        copy.start()
        w2x_sends.append(copy)

    phase("emb_grad")
    grad = functools.reduce(
        lambda a, b: a + b,
        [
            lax.dot_general(pg[i], w1_v[i], (((1,), (1,)), ((), ())), preferred_element_type=F32)
            for i in range(NW)
        ],
    )
    eg_v[...] = grad.astype(BF16)
    phase("docs_sum")
    for k in by_distance(nm):
        src = lax.rem(m + k, nm)
        remote(w2_own, w2_x.at[src], w2x_ss.at[k], w2x_rs.at[src], {"mp": src}).wait_recv()
    w2_sum[0] = functools.reduce(lambda a, b: a + b, [w2_x[i] for i in range(nm)])
    w2_pair = remote(w2_sum.at[0], w2_in, pair_ss.at[2], pair_rs.at[2], {"sub": other})
    w2_pair.start()

    part = planes // 2
    core = plane // part
    mine = lax.rem(plane, part)
    ag_sends = []
    for z in range(2):
        for k in by_distance(planes):
            src = lax.rem(plane + k, planes)
            remote(
                z_s.at[0, 0], z_r.at[z, src], z_ss.at[z, k], z_rs.at[z, src], {"docs": 2 * src + par}
            ).wait_recv()
        z_f[z] = functools.reduce(lambda a, b: a + b, [z_r[z, i].astype(F32) for i in range(planes)]).astype(BF16)

        @pl.when(core == s)
        def _():
            ag_r[s, par, z, mine] = z_f[z]

        for k in by_distance(nd) + [0]:
            copy = remote(
                z_f.at[z], ag_r.at[s, par, z, mine], ag_ss.at[z, k], ag_rs.at[s, par, z, mine],
                {"docs": lax.rem(d + k, nd), "sub": core},
            )
            if k == 0:
                pl.when(core != s)(copy.start)
            else:
                copy.start()
            ag_sends.append((copy, k))
        if z == 0:
            w2_pair.wait_recv()
            w2_sum[1] = w2_sum[0] + w2_in[...]
            w2_z[d] = w2_sum[1]
            w2z_sends = []
            for k in by_distance(nd):
                copy = remote(
                    w2_sum.at[1], w2_z.at[d], w2z_ss.at[k], w2z_rs.at[d], {"docs": lax.rem(d + k, nd)}
                )
                copy.start()
                w2z_sends.append(copy)

    phase("w2_z")
    for k in by_distance(nd):
        src = lax.rem(d + k, nd)
        remote(w2_sum.at[1], w2_z.at[src], w2z_ss.at[k], w2z_rs.at[src], {"docs": src}).wait_recv()
    w2_out[...] = functools.reduce(lambda a, b: a + b, [w2_z[i] for i in range(nd)])

    phase("docs_gather")
    for z in range(2):
        for src in range(NW):
            for k in range(part):
                spot = (src // 2, src % 2, z, k)
                copy = remote(z_f.at[z], ag_r.at[spot], ag_ss.at[z, k], ag_rs.at[spot], {"sub": other})
                same = (src // 2 == s) & (2 * (s * part + k) + src % 2 == d)
                pl.when(jnp.logical_not(same))(copy.wait_recv)
                out_v[k * 16 : k * 16 + 16, pl.ds(src * quarter + z * 128, 128)] = ag_r[spot].astype(F32)
    phase("drain")
    for copy in score_sends + meta_sends + score_relays + meta_relays + [emb_send, emb_pass, w2_pair] + emb_moves + lam_sends + x_sends + w2x_sends + w2z_sends:
        copy.wait_send()
    for copy, to, group in z_sends:
        pl.when(lax.rem(to, 2) == group)(copy.wait_send)
    for copy, k in ag_sends:
        if k == 0:
            pl.when(core != s)(copy.wait_send)
        else:
            copy.wait_send()
    phase(None)


def write_out(a, b, c, a_out, b_out, c_out, sem):
    copies = [pltpu.make_async_copy(x, y, sem.at[i]) for i, (x, y) in enumerate(((a, a_out), (b, b_out), (c, c_out)))]
    for copy in copies:
        copy.start()
    for copy in copies:
        copy.wait()


def solution(mesh):
    nd, nm = mesh.shape["docs"], mesh.shape["mp"]

    def on_device(embeddings, owner_shard, query_local, labels, w_first, w_second):
        rows, width = embeddings.shape
        cap = 2 * rows // nd
        slots = nd * cap
        quarter = width // NW
        tiles = width // nm // 16
        far = nm // 2
        dma = pltpu.SemaphoreType.DMA
        hbm, vmem, anywhere = (pl.BlockSpec(memory_space=a) for a in (pltpu.HBM, pltpu.VMEM, pl.ANY))
        scratch = [
            pltpu.VMEM((rows, width), BF16),
            pltpu.VMEM((1, rows), jnp.int32),
            pltpu.VMEM((1, rows), jnp.int32),
            pltpu.VMEM((1, rows), jnp.int32),
            pltpu.VMEM((NW, width, quarter), BF16),
            pltpu.VMEM((1, width), F32),
            pltpu.VMEM((NW, 1, quarter), F32),
            pltpu.VMEM((rows, width), F32),
            pltpu.VMEM((rows, width), F32),
            pltpu.VMEM((rows, slots), F32),
            pltpu.VMEM((2, slots), BF16),
            pltpu.VMEM((nd, 2, slots), BF16),
            pltpu.VMEM((1, slots), F32),
            pltpu.VMEM((nd, 1, slots), F32),
            pltpu.VMEM((cap, nd, slots), F32),
            pltpu.VMEM((cap, nd, slots), F32),
            pltpu.VMEM((cap, nd, slots), F32),
            pltpu.VMEM((cap, nd, slots), F32),
            pltpu.VMEM((3, rows, width), BF16),
            pltpu.VMEM((nm, width // nm, NW * rows), BF16),
            pltpu.VMEM((NW, rows, quarter), BF16),
            pltpu.VMEM((3, rows, quarter), F32),
            pltpu.VMEM((1, rows), F32),
            pltpu.VMEM((3, 1, rows), F32),
            pltpu.VMEM((nm, width // nm, quarter), F32),
            pltpu.VMEM((2, far, NQ, tiles // 2, 16, 128), BF16),
            pltpu.VMEM((2, far, NQ, tiles // 2, 16, 128), BF16),
            pltpu.VMEM((NQ, tiles // 2, 16, 128), BF16),
            pltpu.VMEM((2, nd // 2, 16, 128), BF16),
            pltpu.VMEM((2, 16, 128), BF16),
            pltpu.VMEM((2, 2, 2, nd // 4, 16, 128), BF16),
            pltpu.VMEM((width // 128, 128), F32),
            pltpu.VMEM((nm, width // 128, 128), F32),
            pltpu.VMEM((2, width // 128, 128), F32),
            pltpu.VMEM((width // 128, 128), F32),
            pltpu.VMEM((nd, width // 128, 128), F32),
            dma((5 + NW,)),
            dma((nd,)),
            dma((nd,)),
            dma((nd,)),
            dma((nd,)),
            dma((3,)),
            dma((3,)),
            dma((EMB,)),
            dma((EMB,)),
            dma((3,)),
            dma((3,)),
            dma((2, far, NQ)),
            dma((2, far, NQ)),
            dma((2, nd // 2)),
            dma((2, nd // 2)),
            dma((2, nd)),
            dma((2, 2, 2, nd // 4)),
            dma((nm,)),
            dma((nm,)),
            dma((nd,)),
            dma((nd,)),
        ]
        shapes = (
            jax.ShapeDtypeStruct((rows, width), BF16),
            jax.ShapeDtypeStruct((width // nm // 2, width), F32),
            jax.ShapeDtypeStruct((width // 128, 128), F32),
        )
        results = pl.pallas_call(
            functools.partial(step_kernel, nd, nm, rows, width, cap),
            out_shape=tuple(pltpu.VMEM(a.shape, a.dtype) for a in shapes),
            in_specs=[hbm] * 6,
            out_specs=(vmem,) * 3,
            scratch_shapes=scratch,
            compiler_params=pltpu.CompilerParams(
                collective_id=0, has_side_effects=True, vmem_limit_bytes=40 * 1024 * 1024
            ),
            name="ranking_step",
        )(
            *(
                pltpu.with_memory_space_constraint(a, pltpu.HBM)
                for a in (
                    embeddings,
                    owner_shard.reshape(1, rows),
                    query_local.reshape(1, rows),
                    labels.reshape(1, rows),
                    w_first,
                    w_second.reshape(1, width),
                )
            )
        )
        emb_grad, w_first_grad, w_second_grad = pl.pallas_call(
            write_out,
            out_shape=shapes,
            in_specs=[anywhere] * 3,
            out_specs=(hbm,) * 3,
            scratch_shapes=[dma((3,))],
            compiler_params=pltpu.CompilerParams(vmem_limit_bytes=1024 * 1024),
            name="write_out",
        )(*results)
        return emb_grad, w_first_grad, w_second_grad.reshape(width)

    whole = ("groups", "docs", "mp", "sub")
    return jax.shard_map(
        on_device,
        mesh=mesh,
        in_specs=(P(whole, None), P(whole, None), P(whole), P(whole), P(), P()),
        out_specs=(P(whole, None), P(("groups", "mp", "sub"), None), P("groups")),
        check_vma=False,
    )
```

```python
import functools
import math

import jax
import jax.numpy as jnp
from jax import lax
from jax.experimental import pallas as pl
from jax.experimental.pallas import tpu as pltpu
from jax.sharding import PartitionSpec as P

MESH = pl.DeviceIdType.MESH
F32 = jnp.float32
BF16 = jnp.bfloat16

NQ = 4
LN2 = math.log(2.0)
NW = 4
EMB = 4


def remote(src, dst, send_sem, recv_sem, where):
    return pltpu.make_async_remote_copy(
        src_ref=src, dst_ref=dst, send_sem=send_sem, recv_sem=recv_sem, device_id=where, device_id_type=MESH
    )


class Phases:
    def __init__(self):
        self.scope = None

    def __call__(self, name):
        if self.scope is not None:
            self.scope.__exit__(None, None, None)
        self.scope = jax.named_scope(name) if name else None
        if self.scope is not None:
            self.scope.__enter__()


def by_distance(count):
    return sorted(range(1, count), key=lambda k: -min(k, count - k))


def step_kernel(
    nd, nm, rows, width, cap,
    emb_h, own_h, qry_h, lab_h, w1_h, w2_h,
    eg_v, out_v, w2_out,
    emb_v, own_v, qry_v, lab_v, w1_v, w2_v, w2_q,
    slope_v, hid_v, hit_v,
    meta_s, meta_r, score_s, score_r,
    sa, sm, sg, sd,
    emb_x, emb_t, pg, slope_x, lam_s, lam_r, g_v,
    x_s, x_r, z_s, z_r, z_f, ag_r,
    w2_own, w2_x, w2_sum, w2_in, w2_z,
    load_sem, meta_ss, meta_rs, score_ss, score_rs,
    pair_ss, pair_rs, emb_ss, emb_rs, lam_ss, lam_rs, x_ss, x_rs, z_ss, z_rs, ag_ss, ag_rs,
    w2x_ss, w2x_rs, w2z_ss, w2z_rs,
):
    d = lax.axis_index("docs")
    m = lax.axis_index("mp")
    s = lax.axis_index("sub")
    other = 1 - s
    slots = nd * cap
    quarter = width // NW
    block_rows = width // nm
    tiles = block_rows // 16
    par = lax.rem(d, 2)
    pair = d + 1 - 2 * par
    mine_q = 2 * s + par

    phase = Phases()
    phase("greet")
    loads = [
        pltpu.make_async_copy(a, b, load_sem.at[i])
        for i, (a, b) in enumerate(
            ((own_h, own_v), (qry_h, qry_v), (lab_h, lab_v), (w2_h, w2_v), (emb_h, emb_v))
        )
    ]
    w_loads = [
        pltpu.make_async_copy(w1_h.at[:, pl.ds(i * quarter, quarter)], w1_v.at[i], load_sem.at[5 + i])
        for i in range(NW)
    ]
    for copy in loads + w_loads:
        copy.start()

    reach = nd // 4
    barrier = pltpu.get_barrier_semaphore()
    near = [k for k in by_distance(nd) if min(k, nd - k) <= reach]
    for k in near:
        pl.semaphore_signal(barrier, inc=1, device_id={"docs": lax.rem(d + k, nd)}, device_id_type=MESH)
    for k in (1, 2, nm - 2, nm - 1):
        pl.semaphore_signal(barrier, inc=1, device_id={"mp": lax.rem(m + k, nm)}, device_id_type=MESH)
    pl.semaphore_signal(barrier, inc=1, device_id={"sub": other}, device_id_type=MESH)
    pl.semaphore_signal(barrier, inc=1, device_id={"docs": pair, "sub": other}, device_id_type=MESH)

    phase("own_slots")
    for copy in loads[:3]:
        copy.wait()
    row_i = lax.broadcasted_iota(jnp.int32, (rows, rows), 0)
    col_i = lax.broadcasted_iota(jnp.int32, (rows, rows), 1)
    eye = row_i == col_i

    def upright(row):
        return jnp.sum(jnp.where(eye, row, 0.0), axis=1, keepdims=True)

    own_row = own_v[...].astype(F32)
    own_col = upright(own_row)
    earlier = jnp.sum(
        jnp.where((own_col == own_row) & (col_i < row_i), 1.0, 0.0), axis=1, keepdims=True
    )
    slot_col = own_col * cap + earlier
    hit = slot_col == lax.broadcasted_iota(jnp.int32, (rows, slots), 1).astype(F32)
    hit_v[...] = jnp.where(hit, 1.0, 0.0)

    def slotted(col):
        return jnp.sum(jnp.where(hit_v[...] > 0.0, col, 0.0), axis=0, keepdims=True)

    mark_own = slotted(upright(qry_v[...].astype(F32)) + 1.0)
    label_own = slotted(upright(lab_v[...].astype(F32)))
    meta_s[0:1, :] = mark_own.astype(BF16)
    meta_s[1:2, :] = label_own.astype(BF16)
    meta_r[0, 0:1, :] = mark_own.astype(BF16)
    meta_r[0, 1:2, :] = label_own.astype(BF16)

    def to_near(src, dst, send_sem, recv_sem):
        copies = []
        for k in near:
            copies.append(remote(src, dst.at[nd - k], send_sem.at[k], recv_sem.at[nd - k], {"docs": lax.rem(d + k, nd)}))
            copies[-1].start()
        return copies

    def from_near(src, dst, send_sem, recv_sem):
        for k in near:
            remote(src, dst.at[k], send_sem.at[k], recv_sem.at[k], {"docs": lax.rem(d + k, nd)}).wait_recv()

    def relays(dst, send_sem, recv_sem):
        ahead, behind = {"docs": lax.rem(d + reach, nd)}, {"docs": lax.rem(d + nd - reach, nd)}
        return [
            remote(
                dst.at[pl.ds(nd - reach, reach)], dst.at[pl.ds(nd - 2 * reach, reach)],
                send_sem.at[nd - 2 * reach], recv_sem.at[nd - 2 * reach], ahead,
            ),
            remote(
                dst.at[pl.ds(1, reach - 1)], dst.at[pl.ds(reach + 1, reach - 1)],
                send_sem.at[reach + 1], recv_sem.at[reach + 1], behind,
            ),
        ]


    phase("scorer")
    for copy in loads[3:] + w_loads:
        copy.wait()
    terms = jnp.zeros((rows, quarter), F32)
    for i in range(NW):
        at = pl.ds(i * quarter, quarter)
        pre = jnp.dot(emb_v[...], w1_v[i], preferred_element_type=F32)
        sig = 0.5 + 0.5 * jnp.tanh(0.5 * pre)
        hid = pre * sig
        hid_v[:, at] = hid
        slope_v[:, at] = sig
        w2_q[i] = w2_v[:, at]
        terms += hid * w2_v[:, at]
    score = jnp.sum(terms, axis=1, keepdims=True)
    score_own = slotted(0.5 * score)
    score_s[...] = score_own
    score_r[0] = score_own
    phase("barrier")
    pl.semaphore_wait(barrier, len(near) + 6)
    phase("send_scores")
    meta_sends = to_near(meta_s, meta_r, meta_ss, meta_rs)
    score_sends = to_near(score_s, score_r, score_ss, score_rs)
    emb_send = remote(emb_v, emb_x.at[0], pair_ss.at[0], pair_rs.at[0], {"sub": other})
    emb_send.start()
    share = rows // EMB
    emb_moves = [
        remote(
            emb_v.at[pl.ds(i * share, share)], emb_x.at[1, pl.ds(i * share, share)],
            emb_ss.at[i], emb_rs.at[i], {"docs": pair},
        )
        for i in range(EMB)
    ]
    for copy in emb_moves[:-1]:
        copy.start()
    phase("near_meta")
    from_near(meta_s, meta_r, meta_ss, meta_rs)
    meta_relays = relays(meta_r, meta_ss, meta_rs)
    for copy in meta_relays:
        copy.start()
    phase("near_wait")
    from_near(score_s, score_r, score_ss, score_rs)
    score_relays = relays(score_r, score_ss, score_rs)
    for copy in score_relays:
        copy.start()

    emb_moves[-1].start()

    phase("turn")
    def turn(block, at):
        for c in range(nm):
            emb_t[c, :, at * rows : (at + 1) * rows] = (
                block[:, c * block_rows : (c + 1) * block_rows].astype(F32).T.astype(BF16)
            )

    def slope_of(i):
        pre = jnp.dot(emb_x[i], w1_v[mine_q], preferred_element_type=F32)
        sig = 0.5 + 0.5 * jnp.tanh(0.5 * pre)
        slope_x[i] = w2_q[mine_q] * (sig + pre * sig * (1.0 - sig))

    turn(emb_v, 0)
    for i in range(NW):
        at = pl.ds(i * quarter, quarter)
        sig = slope_v[:, at]
        slope_v[:, at] = w2_v[:, at] * (sig + hid_v[:, at] * (1.0 - sig))
    emb_send.wait_recv()
    turn(emb_x.at[0], 1)
    slope_of(0)

    phase("meta_wait")
    for copy in meta_relays:
        copy.wait_recv()
    phase("emb_wait")
    for copy in emb_moves:
        copy.wait_recv()
    emb_pass = remote(emb_x.at[1], emb_x.at[2], pair_ss.at[1], pair_rs.at[1], {"sub": other})
    emb_pass.start()
    phase("meta_work")
    lane = lax.broadcasted_iota(jnp.int32, (nd, slots), 1)
    in_group = lax.rem(lane, cap)

    def turned(a, by):
        near = pltpu.roll(a, by, 1)
        far = pltpu.roll(a, by + slots - cap, 1)
        return jnp.where(in_group >= by, near, far)

    mark = jnp.concatenate([meta_r[i, 0:1, :].astype(F32) for i in range(nd)], axis=0)
    label = jnp.concatenate([meta_r[i, 1:2, :].astype(F32) for i in range(nd)], axis=0)
    gain = jnp.exp2(label) - 1.0
    sm[0] = mark
    sg[0] = gain
    packed = 32.0 * mark + gain
    for by in range(1, cap):
        moved = turned(packed, by)
        moved_mark = jnp.floor(moved * (1.0 / 32.0))
        sm[by] = moved_mark
        sg[by] = moved - 32.0 * moved_mark

    group_r = lax.broadcasted_iota(jnp.int32, (slots, slots), 0) // cap
    group_c = lax.broadcasted_iota(jnp.int32, (slots, slots), 1) // cap
    groups = jnp.where(group_r == group_c, 1.0, 0.0).astype(BF16)
    tallies = []
    for q in (1.0, 2.0):
        for least in range(5):
            tallies.append(
                jnp.sum(jnp.where((mark == q) & (label >= float(least)), 1.0, 0.0), axis=0, keepdims=True)
            )
    tallies += [jnp.zeros((6, slots), F32)]
    counts = jnp.dot(jnp.concatenate(tallies, axis=0).astype(BF16), groups, preferred_element_type=F32)
    total = jnp.where(mark == 1.0, counts[0:1], counts[5:6])
    at_least = jnp.where(mark_own == 1.0, counts[1:5], counts[6:10])

    at_least = jnp.concatenate([at_least[:, : slots // 2], at_least[:, slots // 2 :]], axis=0)
    ladders = [jnp.zeros_like(at_least)] * 4
    for r in range(slots):
        ladders[r % 4] = ladders[r % 4] + jnp.where(at_least > float(r), 1.0 / math.log2(2.0 + r), 0.0)
    ladder = (ladders[0] + ladders[1]) + (ladders[2] + ladders[3])
    ladder = jnp.concatenate([ladder[:4], ladder[4:]], axis=1)
    idcg = ladder[0:1] + 2.0 * ladder[1:2] + 4.0 * ladder[2:3] + 8.0 * ladder[3:4]
    inv = jnp.where(idcg > 0.0, 1.0 / jnp.where(idcg > 0.0, idcg, 1.0), 0.0)
    gain_own = jnp.exp2(label_own) - 1.0

    phase("score_wait")
    for copy in score_relays:
        copy.wait_recv()
    phase("soft_rank")
    scores = jnp.concatenate([score_r[i] for i in range(nd)], axis=0)
    sa[0] = scores
    for by in range(1, cap):
        sa[by] = turned(scores, by)

    def soft(by, acc):
        for j in range(nd):
            t = jnp.tanh(sa[by, j : j + 1, :] - scores)
            acc += jnp.where(sm[by, j : j + 1, :] == mark, t, 0.0)
        return acc

    acc = lax.fori_loop(0, cap, soft, jnp.zeros((nd, slots), F32))
    rank = jnp.where(mark > 0.0, 0.5 * (total - 1.0 + acc), 0.0)
    disc = LN2 / jnp.log(2.0 + rank)
    disc_own = disc[0:1, :]
    sd[0] = disc
    for by in range(1, cap):
        sd[by] = turned(disc, by)

    phase("lambdas")
    def pairs(by, acc):
        t = jnp.tanh(sa[by] - score_own)
        gap = sg[by] - gain_own
        term = jnp.abs(sd[by] - disc_own) * (gap - jnp.abs(gap) * t)
        return acc + jnp.where(sm[by] == mark_own, term, 0.0)

    acc = lax.fori_loop(0, cap, pairs, jnp.zeros((nd, slots), F32), unroll=2)
    lam_row = 0.5 * inv * jnp.sum(acc, axis=0, keepdims=True)
    lam = jnp.sum(jnp.where(hit_v[...] > 0.0, lam_row, 0.0), axis=1, keepdims=True)

    phase("pre_grad")
    lam_s[...] = jnp.sum(jnp.where(eye, lam, 0.0), axis=0, keepdims=True)
    quad = ({"sub": other}, {"docs": pair}, {"docs": pair, "sub": other})
    lam_sends = [remote(lam_s, lam_r.at[i], lam_ss.at[i], lam_rs.at[i], where) for i, where in enumerate(quad)]
    for copy in reversed(lam_sends):
        copy.start()
    for i in range(NW):
        pg[i] = (lam * slope_v[:, i * quarter : (i + 1) * quarter]).astype(BF16)
    turn(emb_x.at[1], 2)
    slope_of(1)
    for i in range(width // 128):
        w2_own[i : i + 1, :] = jnp.sum(lam * hid_v[:, i * 128 : (i + 1) * 128], axis=0, keepdims=True)
    w2_z[d] = w2_own[...]
    w2z_sends = []
    for k in by_distance(nd):
        copy = remote(w2_own, w2_z.at[d], w2z_ss.at[k], w2z_rs.at[d], {"docs": lax.rem(d + k, nd)})
        copy.start()
        w2z_sends.append(copy)
    phase("emb_pass_wait")
    emb_pass.wait_recv()
    turn(emb_x.at[2], 3)
    slope_of(2)
    phase("pair_wait")
    for copy in lam_sends:
        copy.wait_recv()
    phase("products")
    both = jnp.concatenate(
        [pg[mine_q]] + [(upright(lam_r[i]) * slope_x[i]).astype(BF16) for i in range(3)], axis=0
    )

    far = nm // 2

    def hop(side, step):
        hops = 2 if step == 0 else 1
        return {"mp": lax.rem(m + (hops if side == 0 else nm - hops), nm)}


    def product(rel):
        g_v[rel] = jnp.dot(emb_t[lax.rem(m + rel, nm)], both, preferred_element_type=F32)

    x_sends = []

    def ring_send(side, step, q, value):
        x_s[side, step, q] = value.astype(BF16)
        copy = remote(
            x_s.at[side, step, q], x_r.at[side, step, q], x_ss.at[side, step, q], x_rs.at[side, step, q],
            hop(side, step),
        )
        copy.start()
        x_sends.append(copy)

    def ring_recv(side, step, q):
        remote(
            x_s.at[side, step, q], x_r.at[side, step, q], x_ss.at[side, step, q], x_rs.at[side, step, q],
            hop(side, step),
        ).wait_recv()
        return x_r[side, step, q].astype(F32)

    def own(rel, q):
        lanes = slice((q % 2) * 128, (q % 2) * 128 + 128)
        return jnp.stack([g_v[rel, e * 16 : e * 16 + 16, lanes] for e in range(q // 2, tiles, 2)])

    def rel_of(side, step):
        away = far - step
        return away if side == 0 else (nm - away) % nm

    def long_way(side, q):
        return (q < NQ // 2) == (side == 0)

    longs = [[q for q in range(NQ) if long_way(side, q)] for side in range(2)]
    shorts = [[q for q in range(NQ) if not long_way(side, q)] for side in range(2)]
    product(far)
    for side in range(2):
        for q in longs[side]:
            ring_send(side, 0, q, own(far, q))
    for side in range(2):
        product(rel_of(side, 1))
        for q in shorts[side] + longs[side]:
            ring_send(side, 1, q, own(rel_of(side, 1), q))
    for step in range(2, far):
        for side in range(2):
            product(rel_of(side, step))
    product(0)

    phase("ring")

    def forward(step, pieces):
        for pair in zip(*pieces):
            for side, q in enumerate(pair):
                block = ring_recv(side, step - 1, q) + own(rel_of(side, step), q)
                if step == 2 and q in longs[side]:
                    block = block + ring_recv(side, 0, q)
                ring_send(side, step, q, block)

    for step in range(2, far):
        forward(step, shorts)
        forward(step, longs)
    order = [q for pair in zip(*longs) for q in pair]

    phase("ring_end")
    z_sends = []
    planes = nd // 2
    plane = d // 2
    for q in order:
        block = own(0, q)
        for side in range(2):
            block = block + ring_recv(side, far - 1, q)
        z_s[q] = block.astype(BF16)
        group, z = q // 2, q % 2

        @pl.when(lax.rem(plane, 2) == group)
        def _():
            z_r[z, plane] = z_s[q, plane // 2]

        for k in by_distance(planes):
            to = lax.rem(plane + k, planes)
            copy = remote(
                z_s.at[q, to // 2], z_r.at[z, plane], z_ss.at[z, k], z_rs.at[z, plane], {"docs": 2 * to + par}
            )
            z_sends.append((copy, to, group))
            pl.when(lax.rem(to, 2) == group)(copy.start)

    for k in by_distance(nd):
        src = lax.rem(d + k, nd)
        remote(w2_own, w2_z.at[src], w2z_ss.at[k], w2z_rs.at[src], {"docs": src}).wait_recv()
    w2_sum[0] = functools.reduce(lambda a, b: a + b, [w2_z[i] for i in range(nd)])
    w2_x[m] = w2_sum[0]
    w2x_sends = []
    for k in by_distance(nm):
        copy = remote(w2_sum.at[0], w2_x.at[m], w2x_ss.at[k], w2x_rs.at[m], {"mp": lax.rem(m + k, nm)})
        copy.start()
        w2x_sends.append(copy)

    phase("emb_grad")
    grad = functools.reduce(
        lambda a, b: a + b,
        [
            lax.dot_general(pg[i], w1_v[i], (((1,), (1,)), ((), ())), preferred_element_type=F32)
            for i in range(NW)
        ],
    )
    eg_v[...] = grad.astype(BF16)
    phase("docs_sum")
    part = planes // 2
    core = plane // part
    mine = lax.rem(plane, part)
    ag_sends = []
    for z in range(2):
        for k in by_distance(planes):
            src = lax.rem(plane + k, planes)
            remote(
                z_s.at[0, 0], z_r.at[z, src], z_ss.at[z, k], z_rs.at[z, src], {"docs": 2 * src + par}
            ).wait_recv()
        z_f[z] = functools.reduce(lambda a, b: a + b, [z_r[z, i].astype(F32) for i in range(planes)]).astype(BF16)

        @pl.when(core == s)
        def _():
            ag_r[s, par, z, mine] = z_f[z]

        for k in by_distance(nd) + [0]:
            copy = remote(
                z_f.at[z], ag_r.at[s, par, z, mine], ag_ss.at[z, k], ag_rs.at[s, par, z, mine],
                {"docs": lax.rem(d + k, nd), "sub": core},
            )
            if k == 0:
                pl.when(core != s)(copy.start)
            else:
                copy.start()
            ag_sends.append((copy, k))
        if z == 0:
            for k in by_distance(nm):
                src = lax.rem(m + k, nm)
                remote(w2_sum.at[0], w2_x.at[src], w2x_ss.at[k], w2x_rs.at[src], {"mp": src}).wait_recv()
            w2_sum[1] = functools.reduce(lambda a, b: a + b, [w2_x[i] for i in range(nm)])
            w2_pair = remote(w2_sum.at[1], w2_in, pair_ss.at[2], pair_rs.at[2], {"sub": other})
            w2_pair.start()

    w2_pair.wait_recv()
    w2_out[...] = w2_sum[1] + w2_in[...]

    phase("docs_gather")
    for z in range(2):
        for src in range(NW):
            for k in range(part):
                spot = (src // 2, src % 2, z, k)
                copy = remote(z_f.at[z], ag_r.at[spot], ag_ss.at[z, k], ag_rs.at[spot], {"sub": other})
                same = (src // 2 == s) & (2 * (s * part + k) + src % 2 == d)
                pl.when(jnp.logical_not(same))(copy.wait_recv)
                out_v[k * 16 : k * 16 + 16, pl.ds(src * quarter + z * 128, 128)] = ag_r[spot].astype(F32)
    phase("drain")
    for copy in score_sends + meta_sends + score_relays + meta_relays + [emb_send, emb_pass, w2_pair] + emb_moves + lam_sends + x_sends + w2x_sends + w2z_sends:
        copy.wait_send()
    for copy, to, group in z_sends:
        pl.when(lax.rem(to, 2) == group)(copy.wait_send)
    for copy, k in ag_sends:
        if k == 0:
            pl.when(core != s)(copy.wait_send)
        else:
            copy.wait_send()
    phase(None)


def write_out(a, b, c, a_out, b_out, c_out, sem):
    copies = [pltpu.make_async_copy(x, y, sem.at[i]) for i, (x, y) in enumerate(((a, a_out), (b, b_out), (c, c_out)))]
    for copy in copies:
        copy.start()
    for copy in copies:
        copy.wait()


def solution(mesh):
    nd, nm = mesh.shape["docs"], mesh.shape["mp"]

    def on_device(embeddings, owner_shard, query_local, labels, w_first, w_second):
        rows, width = embeddings.shape
        cap = 2 * rows // nd
        slots = nd * cap
        quarter = width // NW
        tiles = width // nm // 16
        far = nm // 2
        dma = pltpu.SemaphoreType.DMA
        hbm, vmem, anywhere = (pl.BlockSpec(memory_space=a) for a in (pltpu.HBM, pltpu.VMEM, pl.ANY))
        scratch = [
            pltpu.VMEM((rows, width), BF16),
            pltpu.VMEM((1, rows), jnp.int32),
            pltpu.VMEM((1, rows), jnp.int32),
            pltpu.VMEM((1, rows), jnp.int32),
            pltpu.VMEM((NW, width, quarter), BF16),
            pltpu.VMEM((1, width), F32),
            pltpu.VMEM((NW, 1, quarter), F32),
            pltpu.VMEM((rows, width), F32),
            pltpu.VMEM((rows, width), F32),
            pltpu.VMEM((rows, slots), F32),
            pltpu.VMEM((2, slots), BF16),
            pltpu.VMEM((nd, 2, slots), BF16),
            pltpu.VMEM((1, slots), F32),
            pltpu.VMEM((nd, 1, slots), F32),
            pltpu.VMEM((cap, nd, slots), F32),
            pltpu.VMEM((cap, nd, slots), F32),
            pltpu.VMEM((cap, nd, slots), F32),
            pltpu.VMEM((cap, nd, slots), F32),
            pltpu.VMEM((3, rows, width), BF16),
            pltpu.VMEM((nm, width // nm, NW * rows), BF16),
            pltpu.VMEM((NW, rows, quarter), BF16),
            pltpu.VMEM((3, rows, quarter), F32),
            pltpu.VMEM((1, rows), F32),
            pltpu.VMEM((3, 1, rows), F32),
            pltpu.VMEM((nm, width // nm, quarter), F32),
            pltpu.VMEM((2, far, NQ, tiles // 2, 16, 128), BF16),
            pltpu.VMEM((2, far, NQ, tiles // 2, 16, 128), BF16),
            pltpu.VMEM((NQ, tiles // 2, 16, 128), BF16),
            pltpu.VMEM((2, nd // 2, 16, 128), BF16),
            pltpu.VMEM((2, 16, 128), BF16),
            pltpu.VMEM((2, 2, 2, nd // 4, 16, 128), BF16),
            pltpu.VMEM((width // 128, 128), F32),
            pltpu.VMEM((nm, width // 128, 128), F32),
            pltpu.VMEM((2, width // 128, 128), F32),
            pltpu.VMEM((width // 128, 128), F32),
            pltpu.VMEM((nd, width // 128, 128), F32),
            dma((5 + NW,)),
            dma((nd,)),
            dma((nd,)),
            dma((nd,)),
            dma((nd,)),
            dma((3,)),
            dma((3,)),
            dma((EMB,)),
            dma((EMB,)),
            dma((3,)),
            dma((3,)),
            dma((2, far, NQ)),
            dma((2, far, NQ)),
            dma((2, nd // 2)),
            dma((2, nd // 2)),
            dma((2, nd)),
            dma((2, 2, 2, nd // 4)),
            dma((nm,)),
            dma((nm,)),
            dma((nd,)),
            dma((nd,)),
        ]
        shapes = (
            jax.ShapeDtypeStruct((rows, width), BF16),
            jax.ShapeDtypeStruct((width // nm // 2, width), F32),
            jax.ShapeDtypeStruct((width // 128, 128), F32),
        )
        results = pl.pallas_call(
            functools.partial(step_kernel, nd, nm, rows, width, cap),
            out_shape=tuple(pltpu.VMEM(a.shape, a.dtype) for a in shapes),
            in_specs=[hbm] * 6,
            out_specs=(vmem,) * 3,
            scratch_shapes=scratch,
            compiler_params=pltpu.CompilerParams(
                collective_id=0, has_side_effects=True, vmem_limit_bytes=40 * 1024 * 1024
            ),
            name="ranking_step",
        )(
            *(
                pltpu.with_memory_space_constraint(a, pltpu.HBM)
                for a in (
                    embeddings,
                    owner_shard.reshape(1, rows),
                    query_local.reshape(1, rows),
                    labels.reshape(1, rows),
                    w_first,
                    w_second.reshape(1, width),
                )
            )
        )
        emb_grad, w_first_grad, w_second_grad = pl.pallas_call(
            write_out,
            out_shape=shapes,
            in_specs=[anywhere] * 3,
            out_specs=(hbm,) * 3,
            scratch_shapes=[dma((3,))],
            compiler_params=pltpu.CompilerParams(vmem_limit_bytes=1024 * 1024),
            name="write_out",
        )(*results)
        return emb_grad, w_first_grad, w_second_grad.reshape(width)

    whole = ("groups", "docs", "mp", "sub")
    return jax.shard_map(
        on_device,
        mesh=mesh,
        in_specs=(P(whole, None), P(whole, None), P(whole), P(whole), P(), P()),
        out_specs=(P(whole, None), P(("groups", "mp", "sub"), None), P("groups")),
        check_vma=False,
    )
```
